256 devices in a mesh: cells: 64 (over x, z_lo, y), genes: 4 (over z_hi, core).
Axes of the slice: x: 4, y: 4, z: 8 (z_hi: 2, z_lo: 4; z = z_hi * 4 + z_lo), core: 2. Of those that a mesh axis runs over, the one named last changes fastest.
Arguments:
- counts: int32 [65536, 4096], P('cells', 'genes'), may hold values from 0 to 26, as said below
- library: int32 [65536], P('cells'), may hold values from 2000 to 19999
Outputs:
- adjacency: float32 [4096, 4096], P('cells', 'genes')
- connectivity: float32 [4096], P('cells')
The draws below stay inside these ranges and needn't reach their ends.
Inputs may be any that keep to these rules, and one draw needn't show every extreme that they name: Non-negative integer counts.
All inputs are finite; a program needn't handle non-finite values.
Results may differ from the reference program's by a relative error of at most 0.006.
Values may be sent and summed in bfloat16 or wider, within the bound.
A program may use at most 128 MiB of HBM per device.

```python
import jax
import jax.numpy as jnp
from jax import lax

G = 4096
CELLS_DEV = 1024
CELLS = 65536
N_CELLS = 64


module_count = 32


def draw_counts(key, part):
    module_ids = jax.random.randint(jax.random.fold_in(key, 11), (G,), 0, module_count)
    levels = jax.random.randint(jax.random.fold_in(key, 12), (CELLS, module_count), 0, 8)
    gains = jax.random.randint(jax.random.fold_in(key, 13), (G,), 0, 4)
    noise = jax.random.randint(jax.random.fold_in(key, 14), (CELLS, G), 0, 6)
    present = jax.random.randint(jax.random.fold_in(key, 15), (CELLS, G), 0, 3)
    shared = jnp.take(levels, module_ids, axis=1)
    values = noise + gains[None, :] * shared
    return jnp.where(present > 0, values, 0).astype(jnp.int32)


def place_ends(values, rng, low, high):
    longest = values.shape.index(max(values.shape))
    spots = []
    for shift in (0, 1):
        where = [jax.random.randint(jax.random.fold_in(rng, axis), (), 0, length) for axis, length in enumerate(values.shape)]
        where[longest] = (where[longest] + shift) % values.shape[longest]
        spots.append(tuple(where))
    return values.at[spots[0]].set(low).at[spots[1]].set(high)


def setup_inputs(seed: int = 0) -> dict:
    splits = jax.random.split(jax.random.key(seed), 3)
    return {
        "counts": draw_counts(jax.random.fold_in(splits[2], 71), 0),
        "library": place_ends(jax.random.randint(splits[1], (CELLS,), 2000, 20000), jax.random.fold_in(splits[1], 1), 2000, 19999).astype(jnp.int32),
    }


def normalize(counts, library):
    factor = 10000.0 / library.astype(jnp.float32)
    return jnp.log1p(counts.astype(jnp.float32) * factor[:, None]).astype(jnp.bfloat16)

def reference(counts, library):
    count_blocks = counts.reshape(N_CELLS, CELLS_DEV, G)
    library_blocks = library.reshape(N_CELLS, CELLS_DEV)

    def accumulate(carry, inputs):
        gram, sums, squares = carry
        expressed = normalize(inputs[0], inputs[1]).astype(jnp.float32)
        gram = gram + jnp.dot(expressed.T, expressed, precision=lax.Precision.HIGHEST, preferred_element_type=jnp.float32)
        sums = sums + lax.optimization_barrier(jnp.sum(expressed, axis=0))
        squares = squares + lax.optimization_barrier(jnp.sum(expressed * expressed, axis=0))
        return ((gram, sums, squares), None)
    start = (jnp.zeros((G, G), jnp.float32), jnp.zeros((G,), jnp.float32), jnp.zeros((G,), jnp.float32))
    (gram, sums, squares), unused = lax.scan(accumulate, start, (count_blocks, library_blocks))
    total_cells = float(CELLS)
    means = sums / total_cells
    variances = squares / total_cells - means * means
    scales = lax.rsqrt(variances + 1e-05)
    correlation = (gram / total_cells - means[:, None] * means[None, :]) * scales[:, None] * scales[None, :]
    powered = correlation ** 6
    diagonal = jnp.arange(G)[:, None] == jnp.arange(G)[None, :]
    adjacency = jnp.where(diagonal, jnp.float32(0.0), powered)
    connectivity = lax.optimization_barrier(jnp.sum(adjacency, axis=1))
    return (adjacency, connectivity)
```

```python
import functools

import jax
import jax.numpy as jnp
from jax import lax
from jax.experimental import pallas as pl
from jax.experimental.pallas import tpu as pltpu
from jax.sharding import Mesh
from jax.sharding import PartitionSpec as P

MESH = pl.DeviceIdType.MESH
BLOCK = 1024
SUB = 64
QUARTER = 256
LEVELS = 8190.0
CELLS_ALL = 65536.0


def kernel(
    x_ref, stat_ref, adj_ref, conn_ref,
    xa, xb, rl, tt, f1, d1, r1, f2, d2, r2, zs, zr, ms, mr,
    sz, sx, sy, sc, sq, cm, cu, cw, rowv, cr, csend,
    load_sem, send_sem, recv_sem,
):
    x, zl, y = lax.axis_index("x"), lax.axis_index("zl"), lax.axis_index("y")
    zh, k = lax.axis_index("zh"), lax.axis_index("k")
    z = zh * 4 + zl
    spot = {"x": x, "y": y}
    used = [0]
    started = []

    def remote(src, dst, where, slot=None):
        n = used[0]
        used[0] += 1
        copy = pltpu.make_async_remote_copy(
            src_ref=src,
            dst_ref=dst,
            send_sem=send_sem.at[n],
            recv_sem=recv_sem.at[n if slot is None else slot],
            device_id=where,
            device_id_type=MESH,
        )
        copy.start()
        started.append(copy)
        return copy

    def along_z(hops):
        there = lax.rem(z + hops + 8, 8)
        return {"zh": there // 4, "zl": lax.rem(there, 4)}

    def hop(axis, by):
        return {axis: lax.rem(spot[axis] + by + 4, 4)}

    load = pltpu.make_async_copy(x_ref, xa.at[k], load_sem)
    load.start()
    sz[z] = stat_ref[...]
    stat_z = [remote(stat_ref, sz.at[z], along_z(d)) for d in range(1, 8)]
    load.wait()

    far_half = (1 - zh) * 512

    def leg_one(i):
        return [
            remote(
                xa.at[k, i, pl.ds(far_half + 256 * f, 256)],
                rl.at[f, i],
                along_z(2 - 4 * f),
            )
            for f in range(2)
        ]

    def leg_two(i):
        for c in first_legs[i]:
            c.wait_recv()
        second_legs[i] = [
            remote(rl.at[f, i], xb.at[k, i, pl.ds(256 * f, 256)], along_z(2 - 4 * f))
            for f in range(2)
        ]

    def to_partner(i):
        for c in second_legs[i]:
            c.wait_recv()
        return remote(xb.at[k, i], xb.at[k, i], {"k": 1 - k})

    first_legs, second_legs, partner_b = {}, {}, {}
    first_legs[0], first_legs[1] = leg_one(0), leg_one(1)
    partner_x = remote(xa.at[k], xa.at[k], {"k": 1 - k})

    for c in stat_z:
        c.wait_recv()
    def column(h):
        parts = [(sz[4 * h + i, b : b + 1], sz[4 * h + i, 2 + b : 3 + b]) for i in range(4) for b in range(2)]
        total = functools.reduce(jnp.add, [p[0] for p in parts])
        squares = functools.reduce(jnp.add, [p[1] for p in parts])
        mean = total * (1.0 / 4096.0)
        norms = [p[1] - 2.0 * mean * p[0] + 512.0 * mean * mean for p in parts]
        norm = functools.reduce(jnp.maximum, norms) * 1.0001 + squares * 2.5e-7 + 1e-2
        return total, squares, jnp.sqrt(norm)

    for h in range(2):
        for i, v in enumerate(column(h)):
            sx[x, 4 * h + i : 4 * h + i + 1] = v

    def spread(ref, axis, cells, out, slot):
        here = spot[axis]
        copies = [remote(ref.at[here], ref.at[here], hop(axis, d)) for d in (1, 3, 2)]
        for c in copies:
            c.wait_recv()
        for h in range(2):
            parts = [[ref[i, 4 * h + r : 4 * h + r + 1] for r in range(3)] for i in range(4)]
            total = parts[0][0] + parts[1][0] + parts[2][0] + parts[3][0]
            squares = parts[0][1] + parts[1][1] + parts[2][1] + parts[3][1]
            mean = total * (0.25 / cells)
            norms = [p[2] + (512.0**0.5) * jnp.abs(p[0] * (1.0 / cells) - mean) for p in parts]
            norm = functools.reduce(jnp.maximum, norms)
            for i, v in enumerate((total, squares, norm)):
                out[slot, 4 * h + i : 4 * h + i + 1] = v

    spread(sx, "x", 4096.0, sy, y)
    spread(sy, "y", 16384.0, sc, k)
    other_core = remote(sc.at[k], sc.at[k], {"k": 1 - k})
    leg_two(0)
    other_core.wait_recv()
    for b in range(4):
        h, core = b // 2, b % 2
        rows = sc[core, 4 * h : 4 * h + 4]
        mean = rows[0:1] * (1.0 / CELLS_ALL)
        unit = (LEVELS / 2.0) ** 0.5 / rows[2:3]
        variance = rows[1:2] * (1.0 / CELLS_ALL) - mean * mean
        weight = lax.rsqrt(variance + 1e-05) / unit
        rowv[b, 0:1] = mean
        rowv[b, 1:2] = unit
        rowv[b, 2:3] = weight
        cm[b] = jnp.broadcast_to(mean, (128, BLOCK)).T
        cu[b] = jnp.broadcast_to(unit, (128, BLOCK)).T
    cw[...] = jnp.broadcast_to(rowv[x, 2:3], (128, BLOCK)).T
    mine = 2 * zh + k
    own_mean, own_unit = rowv[mine, 0:1], rowv[mine, 1:2]
    scaled_mean = own_mean * own_unit
    half_sum = stat_ref[pl.ds(zh, 1)]
    for e, total in enumerate((stat_ref[0:1] + stat_ref[1:2], half_sum)):
        sq[e, 0:1] = scaled_mean * (1.0 + e)
        sq[e, 1:2] = total * own_unit * (1.0 + e)
    sq[0, 2:3] = own_unit
    sq[1, 2:3] = own_unit * 2.0

    def products(e, lo):
        depth = 512 if e else 1024
        side = lax.rem(zh + e, 2)
        ones = jnp.ones((depth, 128), jnp.bfloat16)

        def body(t, carry):
            a, hi = t // 2, lax.rem(t, 2)
            left = (xb if e else xa)[a, 2 * lo + hi]
            turned = left.T
            first = pl.multiple_of((2 * hi + lo) * QUARTER, QUARTER)
            mean = cm[2 * side + a, pl.ds(first, QUARTER)]
            unit = cu[2 * side + a, pl.ds(first, QUARTER)]
            total = jnp.dot(turned, ones, preferred_element_type=jnp.float32)
            off = (total - float(depth) * mean) * unit
            mean = mean * unit
            wide = lambda v: jnp.concatenate([v, v], axis=1)
            unit, off, mean = wide(unit), wide(off), wide(mean)
            for q in range(4):
                g = (q % 2) * 2 + q // 2
                if e:
                    right = xa[k, g, pl.ds(pl.multiple_of(zh * 512, 512), 512)]
                else:
                    right = xa[k, g]
                gram = jnp.dot(turned, right, preferred_element_type=jnp.float32)
                at = pl.ds(q * QUARTER, QUARTER)
                value = (
                    gram * unit * sq[e, 2:3, at]
                    - off * sq[e, 0:1, at]
                    - mean * sq[e, 1:2, at]
                )
                value = jnp.clip(value, -LEVELS, LEVELS)
                code = jnp.round(value).astype(jnp.int32).astype(jnp.int16)
                code = code.reshape(4, SUB, QUARTER)
                if q < 2:
                    tt[2 * e + lo, q, t] = code
                else:
                    tt[2 * e + lo, q, :, pl.ds(t, 1)] = code[:, None]
            return carry

        lax.fori_loop(0, 4, body, 0)

    axes = [("x", "y", -1), ("x", "y", 1), ("y", "x", -1), ("y", "x", 1)]

    def at4(axis, by):
        return lax.rem(spot[axis] + by + 4, 4)

    class Ring:
        def __init__(self, tile, axis, s, far, direct, relay):
            self.tile, self.axis, self.s = tile, axis, s
            self.far, self.direct, self.relay = far, direct, relay

        def start(self):
            s = self.s
            self.c_far = remote(
                self.tile(at4(self.axis, 2)), self.far, hop(self.axis, s)
            )
            self.c_direct = remote(
                self.tile(at4(self.axis, -s)), self.direct, hop(self.axis, -s)
            )

        def pass_on(self):
            s = self.s
            self.c_far.wait_recv()
            here = self.tile(at4(self.axis, s))
            here[...] = here[...] + self.far[...]
            self.c_relay = remote(here, self.relay, hop(self.axis, s))

        def total(self):
            self.c_direct.wait_recv()
            self.c_relay.wait_recv()
            here = self.tile(spot[self.axis])
            return here[...] + self.direct[...] + self.relay[...]

    rings1, rings2 = {}, {}

    def p1(j):
        for q, (first, _, s) in enumerate(axes):
            ring = Ring(
                lambda d, q=q: tt.at[j, q, d],
                first, s, f1.at[j, q], d1.at[j, q], r1.at[j, q],
            )
            rings1[j, q] = ring
            ring.start()

    def p2(j):
        for q in range(4):
            rings1[j, q].pass_on()

    def p3(j):
        for q, (first, second, s) in enumerate(axes):
            total = rings1[j, q].total().astype(jnp.int32)
            here = spot[first]
            tt[j, q, here] = ((total + 2) >> 2).astype(jnp.int16)
            ring = Ring(
                lambda d, q=q, here=here: tt.at[j, q, here, d],
                second, s, f2.at[j, q], d2.at[j, q], r2.at[j, q],
            )
            rings2[j, q] = ring
            ring.start()

    def p4(j):
        for q in range(4):
            rings2[j, q].pass_on()

    def p5(j):
        e, lo = j // 2, j % 2
        for q in range(4):
            zs[j, :, q * QUARTER : (q + 1) * QUARTER] = rings2[j, q].total()
        to_x = 2 * lax.rem(zh + e, 2) + x // 2
        to_zl = 2 * lax.rem(x, 2) + lo
        stays = jnp.logical_and(to_x == x, to_zl == zl)
        n = used[0]
        used[0] += 1
        copy = pltpu.make_async_remote_copy(
            src_ref=zs.at[j],
            dst_ref=zr.at[zl],
            send_sem=send_sem.at[n],
            recv_sem=recv_sem.at[LAST + zl],
            device_id={"x": to_x, "zl": to_zl},
            device_id_type=MESH,
        )

        @pl.when(jnp.logical_not(stays))
        def _():
            copy.start()

        @pl.when(stays)
        def _():
            zr[zl] = zs[j]

        last_sends.append((stays, copy))

    last_sends = []

    leg_two(1)
    first_legs[2], first_legs[3] = leg_one(2), leg_one(3)
    partner_x.wait_recv()
    products(0, 0)
    p1(0)
    products(0, 1)
    p1(1)
    p2(0)
    leg_two(2)
    p2(1)
    partner_b[0] = to_partner(0)
    partner_b[1] = to_partner(1)
    p3(0)
    partner_b[0].wait_recv()
    partner_b[1].wait_recv()
    products(1, 0)
    p1(2)
    leg_two(3)
    p3(1)
    p4(0)
    p4(1)
    p2(2)
    p5(0)
    p5(1)
    partner_b[2] = to_partner(2)
    p3(2)
    partner_b[3] = to_partner(3)
    partner_b[2].wait_recv()
    partner_b[3].wait_recv()
    products(1, 1)
    p1(3)
    p4(2)
    p2(3)
    p5(2)
    p3(3)
    p4(3)
    p5(3)

    from_x = 2 * lax.rem(x, 2) + zl // 2
    for s in range(4):
        arrives = jnp.logical_not(jnp.logical_and(from_x == x, zl == s))

        @pl.when(arrives)
        def _(s=s):
            pltpu.make_async_remote_copy(
                src_ref=zs.at[0],
                dst_ref=zr.at[s],
                send_sem=send_sem.at[0],
                recv_sem=recv_sem.at[LAST + s],
                device_id={"x": from_x, "zl": s},
                device_id_type=MESH,
            ).wait_recv()

    value = functools.reduce(lambda a, b: a + b, [zr[s].astype(jnp.int32) for s in range(4)])
    csend[...] = value.astype(jnp.float32)
    crossed = (x // 2) != zh

    mirror = []
    for dz in range(4):
        for dy in range(4):
            there_z, there_y = lax.rem(zl + dz, 4), lax.rem(y + dy, 4)
            n = used[0]
            used[0] += 1
            mirror.append(
                pltpu.make_async_remote_copy(
                    src_ref=ms.at[there_z * 4 + there_y],
                    dst_ref=mr.at[zl * 4 + y],
                    send_sem=send_sem.at[n],
                    recv_sem=recv_sem.at[n],
                    device_id={
                        "x": mine, "zl": there_z, "y": there_y,
                        "zh": x // 2, "k": lax.rem(x, 2),
                    },
                    device_id_type=MESH,
                )
            )

    @pl.when(crossed)
    def _():
        odd = lax.rem(y, 2)
        part = csend[...] * 0.25
        csend[...] = csend[...] * 0.5
        flag = odd.astype(jnp.float32)
        both = jnp.concatenate([part * (1.0 - flag), part * flag], axis=0)
        turned = jnp.round(both.T).astype(jnp.int32).astype(jnp.int16)
        ms[...] = turned.reshape(16, SUB, 128)
        for c in mirror:
            c.start()
        for c in mirror:
            c.wait_recv()
        for m in range(8):
            pair = (mr[2 * m] + mr[2 * m + 1]).astype(jnp.int32)
            at = pl.ds(m * 128, 128)
            csend[:, at] = csend[:, at] + 2.0 * pair.astype(jnp.float32)
        for c in mirror:
            c.wait_send()

    first = pl.multiple_of((zl * 4 + y) * SUB, SUB)
    weight = cw[pl.ds(first, SUB)] * (4.0 / CELLS_ALL)
    row = x * BLOCK + first + lax.broadcasted_iota(jnp.int32, (SUB, 128), 0)
    partial = jnp.zeros((SUB, 128), jnp.float32)
    for m in range(8):
        at = pl.ds(m * 128, 128)
        r = csend[:, at] * weight * rowv[mine, 2:3, at]
        r2_ = r * r
        power = r2_ * r2_ * r2_
        column = mine * BLOCK + m * 128 + lax.broadcasted_iota(jnp.int32, (SUB, 128), 1)
        power = jnp.where(row == column, 0.0, power)
        adj_ref[:, at] = power
        partial = partial + power
    conn_ref[...] = partial
    to = [{"k": 1 - k}, {"zh": 1 - zh}, {"k": 1 - k, "zh": 1 - zh}]
    cr[3] = partial
    ends = [remote(cr.at[3], cr.at[i], where) for i, where in enumerate(to)]
    for c in ends:
        c.wait_recv()
    total = cr[0] + cr[1] + cr[2] + cr[3]
    conn_ref[...] = jnp.broadcast_to(jnp.sum(total, axis=1, keepdims=True), (SUB, 128))
    for c in started:
        c.wait_send()
    for stays, copy in last_sends:

        @pl.when(jnp.logical_not(stays))
        def _(copy=copy):
            copy.wait_send()

    assert used[0] <= LAST, used[0]


LAST = 180


def normalize(counts, library):
    factor = 10000.0 / library.astype(jnp.float32)
    return jnp.log1p(counts.astype(jnp.float32) * factor[:, None]).astype(jnp.bfloat16)


def shards(counts, library):
    own = normalize(counts, library)
    wide = own.astype(jnp.float32).reshape(2, 512, BLOCK)
    halves = jnp.sum(wide, axis=1)
    stats = jnp.concatenate([halves, jnp.sum(wide * wide, axis=1)])
    grouped = own.reshape(BLOCK, 2, 2, QUARTER).transpose(2, 1, 0, 3)
    grouped = grouped.reshape(4, BLOCK, QUARTER)
    i16, f32, bf16 = jnp.int16, jnp.float32, jnp.bfloat16
    vmem = pl.BlockSpec(memory_space=pltpu.VMEM)
    wide_buffer = pltpu.VMEM((4, 4, 4, SUB, QUARTER), i16)
    small_buffer = pltpu.VMEM((4, 4, SUB, QUARTER), i16)
    adjacency, connectivity = pl.pallas_call(
        kernel,
        name="network",
        out_shape=(
            jax.ShapeDtypeStruct((SUB, BLOCK), f32),
            jax.ShapeDtypeStruct((SUB, 128), f32),
        ),
        in_specs=[pl.BlockSpec(memory_space=pl.ANY), vmem],
        out_specs=(vmem, vmem),
        scratch_shapes=[
            pltpu.VMEM((2, 4, BLOCK, QUARTER), bf16),
            pltpu.VMEM((2, 4, 512, QUARTER), bf16),
            pltpu.VMEM((2, 4, QUARTER, QUARTER), bf16),
            pltpu.VMEM((4, 4, 4, 4, SUB, QUARTER), i16),
            wide_buffer, wide_buffer, wide_buffer,
            small_buffer, small_buffer, small_buffer,
            pltpu.VMEM((4, SUB, BLOCK), i16),
            pltpu.VMEM((4, SUB, BLOCK), i16),
            pltpu.VMEM((16, SUB, 128), i16),
            pltpu.VMEM((16, SUB, 128), i16),
            pltpu.VMEM((8, 4, BLOCK), f32),
            pltpu.VMEM((4, 8, BLOCK), f32),
            pltpu.VMEM((4, 8, BLOCK), f32),
            pltpu.VMEM((2, 8, BLOCK), f32),
            pltpu.VMEM((2, 8, BLOCK), f32),
            pltpu.VMEM((4, BLOCK, 128), f32),
            pltpu.VMEM((4, BLOCK, 128), f32),
            pltpu.VMEM((BLOCK, 128), f32),
            pltpu.VMEM((4, 8, BLOCK), f32),
            pltpu.VMEM((4, SUB, 128), f32),
            pltpu.VMEM((SUB, BLOCK), f32),
            pltpu.SemaphoreType.DMA,
            pltpu.SemaphoreType.DMA((LAST,)),
            pltpu.SemaphoreType.DMA((LAST + 4,)),
        ],
        compiler_params=pltpu.CompilerParams(
            has_side_effects=True, vmem_limit_bytes=50 * 1024 * 1024
        ),
    )(grouped, stats)
    return adjacency, connectivity[:, 0]


def solution(mesh):
    names = ("x", "zl", "y", "zh", "k")
    finer = Mesh(mesh.devices.reshape(4, 4, 4, 2, 2), names)
    cells, genes = names[:3], names[3:]
    return jax.shard_map(
        shards,
        mesh=finer,
        in_specs=(P(cells, genes), P(cells)),
        out_specs=(P(cells, genes), P(cells)),
        check_vma=False,
    )
```

```python
import functools

import jax
import jax.numpy as jnp
from jax import lax
from jax.experimental import pallas as pl
from jax.experimental.pallas import tpu as pltpu
from jax.sharding import Mesh
from jax.sharding import PartitionSpec as P

MESH = pl.DeviceIdType.MESH
BLOCK = 1024
SUB = 64
QUARTER = 256
LEVELS = 8190.0
CELLS_ALL = 65536.0


def kernel(
    counts_ref, library_ref, adj_ref, conn_ref,
    raw, xa, xb, gr, gt, tt, f1, d1, r1, f2, d2, r2, zs, zr, ms, mr,
    st, sz, sx, sy, sc, sq, cm, cu, cw, rowv, cr, total_ref,
    load_sem, send_sem, recv_sem,
):
    x, zl, y = lax.axis_index("x"), lax.axis_index("zl"), lax.axis_index("y")
    zh, k = lax.axis_index("zh"), lax.axis_index("k")
    z = zh * 4 + zl
    spot = {"x": x, "y": y}
    mine = 2 * zh + k
    used = [0]
    started = []

    def remote(src, dst, where):
        n = used[0]
        used[0] += 1
        copy = pltpu.make_async_remote_copy(
            src_ref=src,
            dst_ref=dst,
            send_sem=send_sem.at[n],
            recv_sem=recv_sem.at[n],
            device_id=where,
            device_id_type=MESH,
        )
        copy.start()
        started.append(copy)
        return copy

    def along_z(hops):
        there = lax.rem(z + hops + 8, 8)
        return {"zh": there // 4, "zl": lax.rem(there, 4)}

    def hop(axis, by):
        return {axis: lax.rem(spot[axis] + by + 4, 4)}

    barrier = pltpu.get_barrier_semaphore()
    greeted = [along_z(d) for d in range(1, 8)] + [{"k": 1 - k}]
    greeted += [hop(axis, d) for axis in ("x", "y") for d in (1, 2, 3)]
    for where in greeted:
        pl.semaphore_signal(barrier, inc=1, device_id=where, device_id_type=MESH)

    halves = (1 - zh, zh)
    loads = []
    for n in range(4):
        rows = pl.ds(pl.multiple_of(halves[n // 2] * 512 + (n % 2) * 256, 256), 256)
        loads.append(
            (rows, pltpu.make_async_copy(counts_ref.at[rows], raw.at[rows], load_sem.at[n]))
        )
        loads[-1][1].start()
    factor = 10000.0 / library_ref[...].astype(jnp.float32)
    cw[...] = jnp.broadcast_to(factor, (128, BLOCK)).T
    for n in range(4):
        rows, load = loads[n]
        load.wait()
        if n % 2 == 0:
            sq[...] = jnp.zeros_like(sq)

        def piece(i, carry, n=n):
            at = pl.ds(
                pl.multiple_of(halves[n // 2] * 512 + (n % 2) * 256 + i * 64, 64), 64
            )
            scale = cw[at]
            scale = jnp.concatenate([scale, scale], axis=1)
            for g in range(4):
                hi, lo = g % 2, g // 2
                lanes = pl.ds((2 * hi + lo) * QUARTER, QUARTER)
                value = jnp.log1p(raw[at, lanes].astype(jnp.float32) * scale)
                value = value.astype(jnp.bfloat16)
                xa[k, g, at] = value
                value = value.astype(jnp.float32).reshape(8, 8, QUARTER)
                sq[0, :, lanes] = sq[0, :, lanes] + jnp.sum(value, axis=0)
                sq[1, :, lanes] = sq[1, :, lanes] + jnp.sum(value * value, axis=0)
            return carry

        lax.fori_loop(0, 4, piece, 0)
        if n % 2:
            st[pl.ds(halves[n // 2], 1)] = jnp.sum(sq[0], axis=0, keepdims=True)
            st[pl.ds(2 + halves[n // 2], 1)] = jnp.sum(sq[1], axis=0, keepdims=True)
    pl.semaphore_wait(barrier, len(greeted))

    sz[z] = st[...]
    stat_z = [remote(st, sz.at[z], along_z(d)) for d in (4, 3, 5, 2, 6, 1, 7)]
    partner_x = remote(xa.at[k], xa.at[k], {"k": 1 - k})
    far_half = pl.multiple_of((1 - zh) * 512, 512)
    arriving = [
        remote(xa.at[k, i, pl.ds(far_half, 512)], xb.at[k, i], along_z(4))
        for i in range(4)
    ]

    def to_partner(i):
        arriving[i].wait_recv()
        return remote(xb.at[k, i], xb.at[k, i], {"k": 1 - k})

    ones = jnp.ones((BLOCK, 128), jnp.bfloat16)

    def raw_gram(a, lo):
        def body(hi, carry):
            t = 2 * a + hi
            turned = xa[a, 2 * lo + hi].T
            gt[lo, t] = jnp.dot(turned, ones, preferred_element_type=jnp.float32)
            for q in range(4):
                gr[lo, t, :, q * QUARTER : (q + 1) * QUARTER] = jnp.dot(
                    turned,
                    xa[k, (q % 2) * 2 + q // 2],
                    preferred_element_type=jnp.float32,
                )
            return carry

        lax.fori_loop(0, 2, body, 0)

    raw_gram(k, 0)
    raw_gram(k, 1)

    for c in stat_z:
        c.wait_recv()

    def column(h):
        parts = [
            (sz[4 * h + i, b : b + 1], sz[4 * h + i, 2 + b : 3 + b])
            for i in range(4)
            for b in range(2)
        ]
        total = functools.reduce(jnp.add, [p[0] for p in parts])
        squares = functools.reduce(jnp.add, [p[1] for p in parts])
        mean = total * (1.0 / 4096.0)
        norms = [p[1] - 2.0 * mean * p[0] + 512.0 * mean * mean for p in parts]
        norm = functools.reduce(jnp.maximum, norms) * 1.0001 + squares * 2.5e-7 + 1e-2
        return total, squares, jnp.sqrt(norm)

    for h in range(2):
        for i, v in enumerate(column(h)):
            sx[x, 4 * h + i : 4 * h + i + 1] = v

    def spread(ref, axis):
        here = spot[axis]
        return [remote(ref.at[here], ref.at[here], hop(axis, d)) for d in (1, 3, 2)]

    def gathered(copies, ref, cells, out, slot):
        for c in copies:
            c.wait_recv()
        for h in range(2):
            parts = [
                [ref[i, 4 * h + r : 4 * h + r + 1] for r in range(3)] for i in range(4)
            ]
            total = parts[0][0] + parts[1][0] + parts[2][0] + parts[3][0]
            squares = parts[0][1] + parts[1][1] + parts[2][1] + parts[3][1]
            mean = total * (0.25 / cells)
            norms = [
                p[2] + (512.0**0.5) * jnp.abs(p[0] * (1.0 / cells) - mean) for p in parts
            ]
            norm = functools.reduce(jnp.maximum, norms)
            for i, v in enumerate((total, squares, norm)):
                out[slot, 4 * h + i : 4 * h + i + 1] = v

    copies = spread(sx, "x")
    partner_x.wait_recv()
    raw_gram(1 - k, 0)
    gathered(copies, sx, 4096.0, sy, y)
    copies = spread(sy, "y")
    raw_gram(1 - k, 1)
    gathered(copies, sy, 16384.0, sc, k)
    other_core = remote(sc.at[k], sc.at[k], {"k": 1 - k})
    other_core.wait_recv()
    for b in range(4):
        h, core = b // 2, b % 2
        rows = sc[core, 4 * h : 4 * h + 4]
        mean = rows[0:1] * (1.0 / CELLS_ALL)
        unit = (LEVELS / 2.0) ** 0.5 / rows[2:3]
        variance = rows[1:2] * (1.0 / CELLS_ALL) - mean * mean
        rowv[b, 0:1] = mean
        rowv[b, 1:2] = unit
        rowv[b, 2:3] = lax.rsqrt(variance + 1e-05) / unit

    def columns(side):
        for a in range(2):
            b = 2 * side + a
            cm[b] = jnp.broadcast_to(rowv[b, 0:1], (128, BLOCK)).T
            cu[b] = jnp.broadcast_to(rowv[b, 1:2], (128, BLOCK)).T

    columns(zh)
    own_mean, own_unit = rowv[mine, 0:1], rowv[mine, 1:2]
    for e, total in enumerate((st[0:1] + st[1:2], st[pl.ds(zh, 1)])):
        sq[e, 0:1] = own_mean * own_unit * (1.0 + e)
        sq[e, 1:2] = total * own_unit * (1.0 + e)
        sq[e, 2:3] = own_unit * (1.0 + e)

    wide = lambda v: jnp.concatenate([v, v], axis=1)

    def rounded(e, lo, q, a, hi, gram, factors):
        unit, off, mean = factors
        at = pl.ds(q * QUARTER, QUARTER)
        value = (
            gram * unit * sq[e, 2:3, at] - off * sq[e, 0:1, at] - mean * sq[e, 1:2, at]
        )
        value = jnp.clip(value, -LEVELS, LEVELS)
        code = jnp.round(value).astype(jnp.int32).astype(jnp.int16)
        rows = pl.ds(pl.multiple_of(hi * SUB, SUB), SUB)
        for c in range(2):
            part = code[:, c * 128 : (c + 1) * 128].reshape(4, SUB, 128)
            if q < 2:
                tt[2 * e + lo, q, 2 * a + c, :, rows] = part
            else:
                tt[2 * e + lo, q, :, pl.ds(2 * a + c, 1), rows] = part[:, None]

    def row_factors(e, lo, a, hi, total):
        side = lax.rem(zh + e, 2)
        first = pl.multiple_of((2 * hi + lo) * QUARTER, QUARTER)
        mean = cm[2 * side + a, pl.ds(first, QUARTER)]
        unit = cu[2 * side + a, pl.ds(first, QUARTER)]
        off = (total - (512.0 if e else 1024.0) * mean) * unit
        return wide(unit), wide(off), wide(mean * unit)

    def own_codes(lo, q):
        def body(t, carry):
            a, hi = t // 2, lax.rem(t, 2)
            factors = row_factors(0, lo, a, hi, gt[lo, t])
            gram = gr[lo, t, :, q * QUARTER : (q + 1) * QUARTER]
            rounded(0, lo, q, a, hi, gram, factors)
            return carry

        lax.fori_loop(0, 4, body, 0)

    def cross_codes(lo):
        def body(t, carry):
            a, hi = t // 2, lax.rem(t, 2)
            turned = xb[a, 2 * lo + hi].T
            total = jnp.dot(turned, ones[:512], preferred_element_type=jnp.float32)
            factors = row_factors(1, lo, a, hi, total)
            near = pl.ds(pl.multiple_of(zh * 512, 512), 512)
            for q in range(4):
                right = xa[k, (q % 2) * 2 + q // 2, near]
                gram = jnp.dot(turned, right, preferred_element_type=jnp.float32)
                rounded(1, lo, q, a, hi, gram, factors)
            return carry

        lax.fori_loop(0, 4, body, 0)

    axes = [("x", "y", -1), ("x", "y", 1), ("y", "x", -1), ("y", "x", 1)]

    def at4(axis, by):
        return lax.rem(spot[axis] + by + 4, 4)

    class Ring:
        def __init__(self, tile, axis, s, far, direct, relay):
            self.tile, self.axis, self.s = tile, axis, s
            self.far, self.direct, self.relay = far, direct, relay
            self.c_far = remote(tile(at4(axis, 2)), far, hop(axis, s))
            self.c_direct = remote(tile(at4(axis, -s)), direct, hop(axis, -s))

        def pass_on(self):
            self.c_far.wait_recv()
            here = self.tile(at4(self.axis, self.s))
            here[...] = here[...] + self.far[...]
            self.c_relay = remote(here, self.relay, hop(self.axis, self.s))

        def total(self):
            self.c_direct.wait_recv()
            self.c_relay.wait_recv()
            here = self.tile(spot[self.axis])
            return here[...] + self.direct[...] + self.relay[...]

    rings1, rings2 = {}, {}

    def p1(j, q):
        first, _, s = axes[q]
        rings1[j, q] = Ring(
            lambda d: tt.at[j, q, d], first, s, f1.at[j, q], d1.at[j, q], r1.at[j, q]
        )

    def p2(j):
        for q in range(4):
            rings1[j, q].pass_on()

    def p3(j):
        for q, (first, second, s) in enumerate(axes):
            total = rings1[j, q].total().astype(jnp.int32)
            here = spot[first]
            tt[j, q, here] = ((total + 2) >> 2).astype(jnp.int16)
            rings2[j, q] = Ring(
                lambda d, q=q, here=here: tt.at[j, q, here, d],
                second, s, f2.at[j, q], d2.at[j, q], r2.at[j, q],
            )

    def p4(j):
        for q in range(4):
            rings2[j, q].pass_on()

    last_sends = []

    def p5(j):
        e, lo = j // 2, j % 2
        for q in range(4):
            total = rings2[j, q].total()
            for hi in range(2):
                zs[j, hi, :, q * 128 : (q + 1) * 128] = total[hi * SUB : (hi + 1) * SUB]
        to_x = 2 * lax.rem(zh + e, 2) + x // 2
        c = lax.rem(x, 2)
        for hi in range(2):
            to_zl = 2 * hi + lo
            stays = jnp.logical_and(to_x == x, to_zl == zl)
            n = used[0]
            used[0] += 1
            copy = pltpu.make_async_remote_copy(
                src_ref=zs.at[j, hi],
                dst_ref=zr.at[c, zl],
                send_sem=send_sem.at[n],
                recv_sem=recv_sem.at[LAST + c * 4 + zl],
                device_id={"x": to_x, "zl": to_zl},
                device_id_type=MESH,
            )

            @pl.when(jnp.logical_not(stays))
            def _(copy=copy):
                copy.start()

            @pl.when(stays)
            def _(hi=hi):
                zr[c, zl] = zs[j, hi]

            last_sends.append((stays, copy))

    for lo in range(2):
        for q in range(4):
            own_codes(lo, q)
            p1(lo, q)
    columns(1 - zh)
    p2(0)
    p2(1)
    partner_b = [to_partner(0), to_partner(1)]
    p3(0)
    partner_b[0].wait_recv()
    partner_b[1].wait_recv()
    cross_codes(0)
    for q in range(4):
        p1(2, q)
    p3(1)
    p4(0)
    p4(1)
    p2(2)
    p5(0)
    p5(1)
    p3(2)
    cw[...] = jnp.broadcast_to(rowv[x, 2:3], (128, BLOCK)).T
    partner_b += [to_partner(2), to_partner(3)]
    partner_b[2].wait_recv()
    partner_b[3].wait_recv()
    cross_codes(1)
    for q in range(4):
        p1(3, q)
    p4(2)
    p2(3)
    p5(2)
    p3(3)
    p4(3)
    p5(3)

    for c in range(2):
        from_x = 2 * lax.rem(x, 2) + c
        for s in range(4):
            arrives = jnp.logical_not(jnp.logical_and(from_x == x, zl == s))

            @pl.when(arrives)
            def _(c=c, s=s, from_x=from_x):
                pltpu.make_async_remote_copy(
                    src_ref=zs.at[0, 0],
                    dst_ref=zr.at[c, s],
                    send_sem=send_sem.at[0],
                    recv_sem=recv_sem.at[LAST + c * 4 + s],
                    device_id={"x": from_x, "zl": s},
                    device_id_type=MESH,
                ).wait_recv()

    for q in range(4):
        for c in range(2):
            at = slice(q * 128, (q + 1) * 128)
            parts = [zr[c, s, :, at].astype(jnp.int32) for s in range(4)]
            first = q * QUARTER + c * 128
            total_ref[:, first : first + 128] = functools.reduce(jnp.add, parts).astype(
                jnp.float32
            )

    crossed = (x // 2) != zh
    mirror = []
    for dz in (2, 1, 3, 0):
        for dy in (2, 1, 3, 0):
            there_z, there_y = lax.rem(zl + dz, 4), lax.rem(y + dy, 4)
            n = used[0]
            used[0] += 1
            mirror.append(
                pltpu.make_async_remote_copy(
                    src_ref=ms.at[there_z * 4 + there_y],
                    dst_ref=mr.at[zl * 4 + y],
                    send_sem=send_sem.at[n],
                    recv_sem=recv_sem.at[n],
                    device_id={
                        "x": mine, "zl": there_z, "y": there_y,
                        "zh": x // 2, "k": lax.rem(x, 2),
                    },
                    device_id_type=MESH,
                )
            )

    @pl.when(crossed)
    def _():
        low = lax.broadcasted_iota(jnp.int32, (32, 128), 1) < SUB
        for m in range(8):
            part = jnp.round(total_ref[:, m * 128 : (m + 1) * 128] * 0.25)
            top, bottom = part[:32], part[32:]
            even = jnp.where(low, top, pltpu.roll(bottom, SUB, 1))
            odd = jnp.where(low, pltpu.roll(top, SUB, 1), bottom)
            ms[2 * m] = even.astype(jnp.int32).astype(jnp.int16)
            ms[2 * m + 1] = odd.astype(jnp.int32).astype(jnp.int16)
        for c in mirror:
            c.start()
        for c in mirror:
            c.wait_recv()
        for m in range(8):
            pieces = []
            for s in (2 * m, 2 * m + 1):
                part = mr[s].astype(jnp.int32).astype(jnp.float32)
                pieces += [part, pltpu.roll(part, SUB, 1)]
            turned = jnp.concatenate(pieces, axis=0).T[:SUB]
            at = slice(m * 128, (m + 1) * 128)
            total_ref[:, at] = total_ref[:, at] * 0.5 + 2.0 * turned
        for c in mirror:
            c.wait_send()

    first = pl.multiple_of((zl * 4 + y) * SUB, SUB)
    weight = cw[pl.ds(first, SUB)] * (4.0 / CELLS_ALL)
    row = x * BLOCK + first + lax.broadcasted_iota(jnp.int32, (SUB, 128), 0)
    partial = jnp.zeros((SUB, 128), jnp.float32)
    for m in range(8):
        at = pl.ds(m * 128, 128)
        value = total_ref[:, at] * weight * rowv[mine, 2:3, at]
        square = value * value
        power = square * square * square
        lane = mine * BLOCK + m * 128 + lax.broadcasted_iota(jnp.int32, (SUB, 128), 1)
        power = jnp.where(row == lane, 0.0, power)
        adj_ref[:, at] = power
        partial = partial + power
    both = jnp.concatenate([partial, jnp.zeros_like(partial)], axis=0).T
    cr[3] = jnp.broadcast_to(jnp.sum(both, axis=0, keepdims=True), (8, 128))
    to = [{"k": 1 - k}, {"zh": 1 - zh}, {"k": 1 - k, "zh": 1 - zh}]
    ends = [remote(cr.at[3], cr.at[i], where) for i, where in enumerate(to)]
    for c in ends:
        c.wait_recv()
    conn_ref[...] = cr[0] + cr[1] + cr[2] + cr[3]
    for c in started:
        c.wait_send()
    for stays, copy in last_sends:

        @pl.when(jnp.logical_not(stays))
        def _(copy=copy):
            copy.wait_send()

    assert used[0] <= LAST, used[0]


LAST = 170


def shards(counts, library):
    i16, f32, bf16 = jnp.int16, jnp.float32, jnp.bfloat16
    vmem = pl.BlockSpec(memory_space=pltpu.VMEM)
    wide_buffer = pltpu.VMEM((4, 4, 4, 128, 128), i16)
    small_buffer = pltpu.VMEM((4, 4, 128, 128), i16)
    adjacency, connectivity = pl.pallas_call(
        kernel,
        name="network",
        out_shape=(
            jax.ShapeDtypeStruct((SUB, BLOCK), f32),
            jax.ShapeDtypeStruct((8, 128), f32),
        ),
        in_specs=[pl.BlockSpec(memory_space=pl.ANY), vmem],
        out_specs=(vmem, vmem),
        scratch_shapes=[
            pltpu.VMEM((BLOCK, BLOCK), jnp.int32),
            pltpu.VMEM((2, 4, BLOCK, QUARTER), bf16),
            pltpu.VMEM((2, 4, 512, QUARTER), bf16),
            pltpu.VMEM((2, 4, QUARTER, BLOCK), f32),
            pltpu.VMEM((2, 4, QUARTER, 128), f32),
            pltpu.VMEM((4, 4, 4, 4, 128, 128), i16),
            wide_buffer, wide_buffer, wide_buffer,
            small_buffer, small_buffer, small_buffer,
            pltpu.VMEM((4, 2, SUB, 512), i16),
            pltpu.VMEM((2, 4, SUB, 512), i16),
            pltpu.VMEM((16, 32, 128), i16),
            pltpu.VMEM((16, 32, 128), i16),
            pltpu.VMEM((4, BLOCK), f32),
            pltpu.VMEM((8, 4, BLOCK), f32),
            pltpu.VMEM((4, 8, BLOCK), f32),
            pltpu.VMEM((4, 8, BLOCK), f32),
            pltpu.VMEM((2, 8, BLOCK), f32),
            pltpu.VMEM((2, 8, BLOCK), f32),
            pltpu.VMEM((4, BLOCK, 128), f32),
            pltpu.VMEM((4, BLOCK, 128), f32),
            pltpu.VMEM((BLOCK, 128), f32),
            pltpu.VMEM((4, 8, BLOCK), f32),
            pltpu.VMEM((4, 8, 128), f32),
            pltpu.VMEM((SUB, BLOCK), f32),
            pltpu.SemaphoreType.DMA((4,)),
            pltpu.SemaphoreType.DMA((LAST,)),
            pltpu.SemaphoreType.DMA((LAST + 8,)),
        ],
        compiler_params=pltpu.CompilerParams(
            collective_id=0, has_side_effects=True, vmem_limit_bytes=56 * 1024 * 1024
        ),
    )(counts, library.reshape(1, BLOCK))
    return adjacency, connectivity[0, :SUB]


def solution(mesh):
    names = ("x", "zl", "y", "zh", "k")
    finer = Mesh(mesh.devices.reshape(4, 4, 4, 2, 2), names)
    cells, genes = names[:3], names[3:]
    return jax.shard_map(
        shards,
        mesh=finer,
        in_specs=(P(cells, genes), P(cells)),
        out_specs=(P(cells, genes), P(cells)),
        check_vma=False,
    )
```

```python
import functools

import jax
import jax.numpy as jnp
from jax import lax
from jax.experimental import pallas as pl
from jax.experimental.pallas import tpu as pltpu
from jax.sharding import Mesh
from jax.sharding import PartitionSpec as P

MESH = pl.DeviceIdType.MESH
BLOCK = 1024
SUB = 64
QUARTER = 256
LEVELS = 8190.0
CELLS_ALL = 65536.0


def kernel(
    counts_ref, library_ref, adj_ref, conn_ref,
    raw, xa, xb, rl, gr, gt, tt, f1, d1, r1, f2, d2, r2, zs, zr, xs, xr, ms, mr,
    st, sz, sx, sy, sc, sq, cm, cu, cw, rowv, cr, total_ref,
    load_sem, send_sem, recv_sem,
):
    x, zl, y = lax.axis_index("x"), lax.axis_index("zl"), lax.axis_index("y")
    zh, k = lax.axis_index("zh"), lax.axis_index("k")
    z = zh * 4 + zl
    spot = {"x": x, "y": y}
    mine = 2 * zh + k
    used = [0]
    started = []

    def remote(src, dst, where):
        n = used[0]
        used[0] += 1
        copy = pltpu.make_async_remote_copy(
            src_ref=src,
            dst_ref=dst,
            send_sem=send_sem.at[n],
            recv_sem=recv_sem.at[n],
            device_id=where,
            device_id_type=MESH,
        )
        copy.start()
        started.append(copy)
        return copy

    def along_z(hops):
        there = lax.rem(z + hops + 8, 8)
        return {"zh": there // 4, "zl": lax.rem(there, 4)}

    def hop(axis, by):
        return {axis: lax.rem(spot[axis] + by + 4, 4)}

    barrier = pltpu.get_barrier_semaphore()
    half_z = [{"zl": lax.rem(zl + d, 4)} for d in (3, 1, 2)]
    greeted = half_z + [{"k": 1 - k}, {"zh": 1 - zh}, {"zh": 1 - zh, "k": 1 - k}]
    greeted += [along_z(2), along_z(-2)]
    greeted += [hop(axis, d) for axis in ("x", "y") for d in (1, 2, 3)]
    for where in greeted:
        pl.semaphore_signal(barrier, inc=1, device_id=where, device_id_type=MESH)

    halves = (1 - zh, zh)
    loads = []
    for n in range(4):
        rows = pl.ds(pl.multiple_of(halves[n // 2] * 512 + (n % 2) * 256, 256), 256)
        loads.append(
            (rows, pltpu.make_async_copy(counts_ref.at[rows], raw.at[rows], load_sem.at[n]))
        )
        loads[-1][1].start()
    factor = 10000.0 / library_ref[...].astype(jnp.float32)
    cw[...] = jnp.broadcast_to(factor, (128, BLOCK)).T
    for n in range(4):
        rows, load = loads[n]
        load.wait()
        if n % 2 == 0:
            sq[...] = jnp.zeros_like(sq)

        def piece(i, carry, n=n):
            at = pl.ds(
                pl.multiple_of(halves[n // 2] * 512 + (n % 2) * 256 + i * 64, 64), 64
            )
            scale = cw[at]
            scale = jnp.concatenate([scale, scale], axis=1)
            for g in range(4):
                hi, lo = g % 2, g // 2
                lanes = pl.ds((2 * hi + lo) * QUARTER, QUARTER)
                value = jnp.log1p(raw[at, lanes].astype(jnp.float32) * scale)
                value = value.astype(jnp.bfloat16)
                xa[k, g, at] = value
                value = value.astype(jnp.float32).reshape(8, 8, QUARTER)
                sq[0, :, lanes] = sq[0, :, lanes] + jnp.sum(value, axis=0)
                sq[1, :, lanes] = sq[1, :, lanes] + jnp.sum(value * value, axis=0)
            return carry

        lax.fori_loop(0, 4, piece, 0)
        if n % 2:
            st[pl.ds(halves[n // 2], 1)] = jnp.sum(sq[0], axis=0, keepdims=True)
            st[pl.ds(2 + halves[n // 2], 1)] = jnp.sum(sq[1], axis=0, keepdims=True)
    pl.semaphore_wait(barrier, len(greeted))

    sz[zl] = st[...]
    stat_z = [remote(st, sz.at[zl], where) for where in half_z]
    partner_x = remote(xa.at[k], xa.at[k], {"k": 1 - k})
    far_half = pl.multiple_of((1 - zh) * 512, 512)

    ways = (along_z(2), along_z(-2))
    leg_one, leg_two = {}, {}

    def send_genes(i):
        leg_one[i] = [
            remote(
                xa.at[k, i, pl.ds(pl.multiple_of(far_half + 256 * f, 256), 256)],
                rl.at[f, i],
                ways[f],
            )
            for f in range(2)
        ]

    def forward(i):
        for c in leg_one[i]:
            c.wait_recv()
        leg_two[i] = [
            remote(rl.at[f, i], xb.at[k, i, pl.ds(256 * f, 256)], ways[f])
            for f in range(2)
        ]

    send_genes(0)
    send_genes(1)

    def to_partner(i):
        for c in leg_two[i]:
            c.wait_recv()
        return remote(xb.at[k, i], xb.at[k, i], {"k": 1 - k})

    ones = jnp.ones((BLOCK, 128), jnp.bfloat16)

    def raw_gram(a, lo):
        def body(hi, carry):
            t = 2 * a + hi
            turned = xa[a, 2 * lo + hi].T
            gt[lo, t] = jnp.dot(turned, ones, preferred_element_type=jnp.float32)
            for q in range(4):
                gr[lo, t, :, q * QUARTER : (q + 1) * QUARTER] = jnp.dot(
                    turned,
                    xa[k, (q % 2) * 2 + q // 2],
                    preferred_element_type=jnp.float32,
                )
            return carry

        lax.fori_loop(0, 2, body, 0)

    raw_gram(k, 0)
    raw_gram(k, 1)

    for c in stat_z:
        c.wait_recv()

    parts = [(sz[i, b : b + 1], sz[i, 2 + b : 3 + b]) for i in range(4) for b in range(2)]
    total = functools.reduce(jnp.add, [p[0] for p in parts])
    squares = functools.reduce(jnp.add, [p[1] for p in parts])
    mean = total * (1.0 / 4096.0)
    norms = [p[1] - 2.0 * mean * p[0] + 512.0 * mean * mean for p in parts]
    norm = functools.reduce(jnp.maximum, norms) * 1.0001 + squares * 2.5e-7 + 1e-2
    for i, v in enumerate((total, squares, jnp.sqrt(norm))):
        sx[x, i : i + 1] = v

    def spread(ref, axis):
        here = spot[axis]
        return [remote(ref.at[here], ref.at[here], hop(axis, d)) for d in (1, 3, 2)]

    def gathered(copies, ref, cells, out, slot):
        for c in copies:
            c.wait_recv()
        parts = [[ref[i, r : r + 1] for r in range(3)] for i in range(4)]
        total = parts[0][0] + parts[1][0] + parts[2][0] + parts[3][0]
        squares = parts[0][1] + parts[1][1] + parts[2][1] + parts[3][1]
        mean = total * (0.25 / cells)
        norms = [
            p[2] + (512.0**0.5) * jnp.abs(p[0] * (1.0 / cells) - mean) for p in parts
        ]
        norm = functools.reduce(jnp.maximum, norms)
        for i, v in enumerate((total, squares, norm)):
            out[slot, i : i + 1] = v

    copies = spread(sx, "x")
    partner_x.wait_recv()
    forward(0)
    raw_gram(1 - k, 0)
    gathered(copies, sx, 4096.0, sy, y)
    copies = spread(sy, "y")
    raw_gram(1 - k, 1)
    gathered(copies, sy, 16384.0, sc, mine)
    stat_core = remote(sc.at[mine], sc.at[mine], {"k": 1 - k})
    stat_far = [
        remote(sc.at[mine], sc.at[mine], {"zh": 1 - zh}),
        remote(sc.at[mine], sc.at[mine], {"zh": 1 - zh, "k": 1 - k}),
    ]
    forward(1)
    send_genes(2)
    send_genes(3)

    def columns(side):
        for a in range(2):
            b = 2 * side + a
            mean = sc[b, 0:1] * (1.0 / CELLS_ALL)
            unit = (LEVELS / 2.0) ** 0.5 / sc[b, 2:3]
            variance = sc[b, 1:2] * (1.0 / CELLS_ALL) - mean * mean
            rowv[b, 0:1] = mean
            rowv[b, 1:2] = unit
            rowv[b, 2:3] = lax.rsqrt(variance + 1e-05) / unit
            cm[b] = jnp.broadcast_to(mean, (128, BLOCK)).T
            cu[b] = jnp.broadcast_to(unit, (128, BLOCK)).T

    stat_core.wait_recv()
    columns(zh)
    own_mean, own_unit = rowv[mine, 0:1], rowv[mine, 1:2]
    for e, total in enumerate((st[0:1] + st[1:2], st[pl.ds(zh, 1)])):
        sq[e, 0:1] = own_mean * own_unit * (1.0 + e)
        sq[e, 1:2] = total * own_unit * (1.0 + e)
        sq[e, 2:3] = own_unit * (1.0 + e)

    wide = lambda v: jnp.concatenate([v, v], axis=1)

    def rounded(e, lo, q, a, hi, gram, factors):
        unit, off, mean = factors
        at = pl.ds(q * QUARTER, QUARTER)
        value = (
            gram * unit * sq[e, 2:3, at] - off * sq[e, 0:1, at] - mean * sq[e, 1:2, at]
        )
        value = jnp.clip(value, -LEVELS, LEVELS)
        code = jnp.round(value).astype(jnp.int32).astype(jnp.int16)
        rows = pl.ds(pl.multiple_of(hi * SUB, SUB), SUB)
        for c in range(2):
            part = code[:, c * 128 : (c + 1) * 128].reshape(4, SUB, 128)
            if q < 2:
                tt[2 * e + lo, q, 2 * a + c, :, rows] = part
            else:
                tt[2 * e + lo, q, :, pl.ds(2 * a + c, 1), rows] = part[:, None]

    def row_factors(e, lo, a, hi, total):
        side = lax.rem(zh + e, 2)
        first = pl.multiple_of((2 * hi + lo) * QUARTER, QUARTER)
        mean = cm[2 * side + a, pl.ds(first, QUARTER)]
        unit = cu[2 * side + a, pl.ds(first, QUARTER)]
        off = (total - (512.0 if e else 1024.0) * mean) * unit
        return wide(unit), wide(off), wide(mean * unit)

    def own_codes(lo, q):
        def body(t, carry):
            a, hi = t // 2, lax.rem(t, 2)
            factors = row_factors(0, lo, a, hi, gt[lo, t])
            gram = gr[lo, t, :, q * QUARTER : (q + 1) * QUARTER]
            rounded(0, lo, q, a, hi, gram, factors)
            return carry

        lax.fori_loop(0, 4, body, 0)

    def cross_codes(lo):
        def body(t, carry):
            a, hi = t // 2, lax.rem(t, 2)
            turned = xb[a, 2 * lo + hi].T
            total = jnp.dot(turned, ones[:512], preferred_element_type=jnp.float32)
            factors = row_factors(1, lo, a, hi, total)
            near = pl.ds(pl.multiple_of(zh * 512, 512), 512)
            for q in range(4):
                right = xa[k, (q % 2) * 2 + q // 2, near]
                gram = jnp.dot(turned, right, preferred_element_type=jnp.float32)
                rounded(1, lo, q, a, hi, gram, factors)
            return carry

        lax.fori_loop(0, 4, body, 0)

    axes = [("x", "y", -1), ("x", "y", 1), ("y", "x", -1), ("y", "x", 1)]

    def at4(axis, by):
        return lax.rem(spot[axis] + by + 4, 4)

    class Ring:
        def __init__(self, tile, axis, s, far, direct, relay):
            self.tile, self.axis, self.s = tile, axis, s
            self.far, self.direct, self.relay = far, direct, relay
            self.c_far = remote(tile(at4(axis, 2)), far, hop(axis, s))

        def send_direct(self):
            s = self.s
            self.c_direct = remote(
                self.tile(at4(self.axis, -s)), self.direct, hop(self.axis, -s)
            )

        def pass_on(self):
            self.c_far.wait_recv()
            here = self.tile(at4(self.axis, self.s))
            here[...] = here[...] + self.far[...]
            self.c_relay = remote(here, self.relay, hop(self.axis, self.s))

        def total(self):
            self.c_direct.wait_recv()
            self.c_relay.wait_recv()
            here = self.tile(spot[self.axis])
            return here[...] + self.direct[...] + self.relay[...]

    rings1, rings2 = {}, {}

    def p1(j, q):
        first, _, s = axes[q]
        rings1[j, q] = Ring(
            lambda d: tt.at[j, q, d], first, s, f1.at[j, q], d1.at[j, q], r1.at[j, q]
        )

    def p2(j):
        for q in range(4):
            rings1[j, q].pass_on()

    def p3(j):
        for q, (first, second, s) in enumerate(axes):
            total = rings1[j, q].total().astype(jnp.int32)
            here = spot[first]
            tt[j, q, here] = ((total + 2) >> 2).astype(jnp.int16)
            rings2[j, q] = Ring(
                lambda d, q=q, here=here: tt.at[j, q, here, d],
                second, s, f2.at[j, q], d2.at[j, q], r2.at[j, q],
            )
        for q in range(4):
            rings2[j, q].send_direct()

    def p4(j):
        for q in range(4):
            rings2[j, q].pass_on()

    last_sends = []

    def p5(j):
        e, lo = j // 2, j % 2
        for q in range(4):
            total = rings2[j, q].total()
            for hi in range(2):
                zs[j, hi, :, q * 128 : (q + 1) * 128] = total[hi * SUB : (hi + 1) * SUB]
        for hi in range(2):
            hand_over(zs.at[j, hi], zr.at[e, zl], {"zl": 2 * hi + lo}, 2 * hi + lo == zl, e * 4 + zl)

    def hand_over(src, dst, where, stays, slot):
        n = used[0]
        used[0] += 1
        copy = pltpu.make_async_remote_copy(
            src_ref=src,
            dst_ref=dst,
            send_sem=send_sem.at[n],
            recv_sem=recv_sem.at[LAST + slot],
            device_id=where,
            device_id_type=MESH,
        )

        @pl.when(jnp.logical_not(stays))
        def _():
            copy.start()

        @pl.when(stays)
        def _():
            dst[...] = src[...]

        last_sends.append((stays, copy))

    def arrival(src, dst, slot):
        return pltpu.make_async_remote_copy(
            src_ref=src,
            dst_ref=dst,
            send_sem=send_sem.at[0],
            recv_sem=recv_sem.at[LAST + slot],
            device_id={"k": 1 - k},
            device_id_type=MESH,
        )

    c_here = lax.rem(x, 2)

    def settle(e):
        for s in range(4):

            @pl.when(zl != s)
            def _(s=s):
                arrival(zs.at[0, 0], zr.at[e, s], e * 4 + s).wait_recv()

        for q in range(4):
            at = slice(q * 128, (q + 1) * 128)
            parts = [zr[e, s, :, at].astype(jnp.int32) for s in range(4)]
            code = (functools.reduce(jnp.add, parts) + 2) >> 2
            xs[e, :, at] = code.astype(jnp.int16)
            if e:
                low = lax.broadcasted_iota(jnp.int32, (32, 128), 1) < SUB
                part = code.astype(jnp.float32)
                top, bottom = part[:32], part[32:]
                even = jnp.where(low, top, pltpu.roll(bottom, SUB, 1))
                odd = jnp.where(low, pltpu.roll(top, SUB, 1), bottom)
                for half, v in enumerate((even, odd)):
                    ms[2 * q + half] = v.astype(jnp.int32).astype(jnp.int16)
        if e:
            for n in range(8):
                slot = used[0]
                used[0] += 1
                copy = pltpu.make_async_remote_copy(
                    src_ref=ms.at[n],
                    dst_ref=mr.at[zl * 4 + y],
                    send_sem=send_sem.at[slot],
                    recv_sem=recv_sem.at[LAST + 10 + zl * 4 + y],
                    device_id={
                        "x": mine, "zl": n // 2, "y": 2 * c_here + n % 2,
                        "zh": 1 - zh, "k": x // 2,
                    },
                    device_id_type=MESH,
                )
                copy.start()
                started.append(copy)
        to_x = 2 * lax.rem(zh + e, 2) + x // 2
        hand_over(xs.at[e], xr.at[c_here], {"x": to_x}, to_x == x, 8 + c_here)

    def directs(j):
        for q in range(4):
            rings1[j, q].send_direct()

    for lo in range(2):
        for q in range(4):
            own_codes(lo, q)
            p1(lo, q)
        directs(lo)
    p2(0)
    partner_b = [to_partner(0), to_partner(1)]
    for c in stat_far:
        c.wait_recv()
    columns(1 - zh)
    p2(1)
    forward(2)
    partner_b[0].wait_recv()
    partner_b[1].wait_recv()
    cross_codes(0)
    for q in range(4):
        p1(2, q)
    directs(2)
    p3(0)
    forward(3)
    cw[...] = jnp.broadcast_to(rowv[x, 2:3], (128, BLOCK)).T
    p3(1)
    p4(0)
    p2(2)
    p4(1)
    partner_b += [to_partner(2)]
    p5(0)
    partner_b += [to_partner(3)]
    p5(1)
    partner_b[2].wait_recv()
    partner_b[3].wait_recv()
    cross_codes(1)
    for q in range(4):
        p1(3, q)
    directs(3)
    p3(2)
    settle(0)
    p2(3)
    p4(2)
    p3(3)
    p5(2)
    p4(3)
    p5(3)

    settle(1)

    for c in range(2):

        @pl.when(2 * lax.rem(x, 2) + c != x)
        def _(c=c):
            arrival(xs.at[0], xr.at[c], 8 + c).wait_recv()

        for q in range(4):
            first = q * QUARTER + c * 128
            part = xr[c, :, q * 128 : (q + 1) * 128].astype(jnp.int32)
            total_ref[:, first : first + 128] = 4.0 * part.astype(jnp.float32)

    @pl.when((x // 2) != zh)
    def _():
        for s in range(16):
            arrival(ms.at[0], mr.at[s], 10 + s).wait_recv()
        for m in range(8):
            pieces = []
            for s in (2 * m, 2 * m + 1):
                part = mr[s].astype(jnp.int32).astype(jnp.float32)
                pieces += [part, pltpu.roll(part, SUB, 1)]
            turned = jnp.concatenate(pieces, axis=0).T[:SUB]
            at = slice(m * 128, (m + 1) * 128)
            total_ref[:, at] = total_ref[:, at] * 0.5 + 2.0 * turned

    first = pl.multiple_of((zl * 4 + y) * SUB, SUB)
    weight = cw[pl.ds(first, SUB)] * (4.0 / CELLS_ALL)
    row = x * BLOCK + first + lax.broadcasted_iota(jnp.int32, (SUB, 128), 0)
    partial = jnp.zeros((SUB, 128), jnp.float32)
    for m in range(8):
        at = pl.ds(m * 128, 128)
        value = total_ref[:, at] * weight * rowv[mine, 2:3, at]
        square = value * value
        power = square * square * square
        lane = mine * BLOCK + m * 128 + lax.broadcasted_iota(jnp.int32, (SUB, 128), 1)
        power = jnp.where(row == lane, 0.0, power)
        adj_ref[:, at] = power
        partial = partial + power
    both = jnp.concatenate([partial, jnp.zeros_like(partial)], axis=0).T
    cr[3] = jnp.broadcast_to(jnp.sum(both, axis=0, keepdims=True), (8, 128))
    to = [{"k": 1 - k}, {"zh": 1 - zh}, {"k": 1 - k, "zh": 1 - zh}]
    ends = [remote(cr.at[3], cr.at[i], where) for i, where in enumerate(to)]
    for c in ends:
        c.wait_recv()
    conn_ref[...] = cr[0] + cr[1] + cr[2] + cr[3]
    for c in started:
        c.wait_send()
    for stays, copy in last_sends:

        @pl.when(jnp.logical_not(stays))
        def _(copy=copy):
            copy.wait_send()

    assert used[0] <= LAST, used[0]


LAST = 190


def shards(counts, library):
    i16, f32, bf16 = jnp.int16, jnp.float32, jnp.bfloat16
    vmem = pl.BlockSpec(memory_space=pltpu.VMEM)
    wide_buffer = pltpu.VMEM((4, 4, 4, 128, 128), i16)
    small_buffer = pltpu.VMEM((4, 4, 128, 128), i16)
    adjacency, connectivity = pl.pallas_call(
        kernel,
        name="network",
        out_shape=(
            jax.ShapeDtypeStruct((SUB, BLOCK), f32),
            jax.ShapeDtypeStruct((8, 128), f32),
        ),
        in_specs=[pl.BlockSpec(memory_space=pl.ANY), vmem],
        out_specs=(vmem, vmem),
        scratch_shapes=[
            pltpu.VMEM((BLOCK, BLOCK), jnp.int32),
            pltpu.VMEM((2, 4, BLOCK, QUARTER), bf16),
            pltpu.VMEM((2, 4, 512, QUARTER), bf16),
            pltpu.VMEM((2, 4, QUARTER, QUARTER), bf16),
            pltpu.VMEM((2, 4, QUARTER, BLOCK), f32),
            pltpu.VMEM((2, 4, QUARTER, 128), f32),
            pltpu.VMEM((4, 4, 4, 4, 128, 128), i16),
            wide_buffer, wide_buffer, wide_buffer,
            small_buffer, small_buffer, small_buffer,
            pltpu.VMEM((4, 2, SUB, 512), i16),
            pltpu.VMEM((2, 4, SUB, 512), i16),
            pltpu.VMEM((2, SUB, 512), i16),
            pltpu.VMEM((2, SUB, 512), i16),
            pltpu.VMEM((8, 32, 128), i16),
            pltpu.VMEM((16, 32, 128), i16),
            pltpu.VMEM((4, BLOCK), f32),
            pltpu.VMEM((4, 4, BLOCK), f32),
            pltpu.VMEM((4, 4, BLOCK), f32),
            pltpu.VMEM((4, 4, BLOCK), f32),
            pltpu.VMEM((4, 4, BLOCK), f32),
            pltpu.VMEM((2, 8, BLOCK), f32),
            pltpu.VMEM((4, BLOCK, 128), f32),
            pltpu.VMEM((4, BLOCK, 128), f32),
            pltpu.VMEM((BLOCK, 128), f32),
            pltpu.VMEM((4, 8, BLOCK), f32),
            pltpu.VMEM((4, 8, 128), f32),
            pltpu.VMEM((SUB, BLOCK), f32),
            pltpu.SemaphoreType.DMA((4,)),
            pltpu.SemaphoreType.DMA((LAST,)),
            pltpu.SemaphoreType.DMA((LAST + 26,)),
        ],
        compiler_params=pltpu.CompilerParams(
            collective_id=0, has_side_effects=True, vmem_limit_bytes=56 * 1024 * 1024
        ),
    )(counts, library.reshape(1, BLOCK))
    return adjacency, connectivity[0, :SUB]


def solution(mesh):
    names = ("x", "zl", "y", "zh", "k")
    finer = Mesh(mesh.devices.reshape(4, 4, 4, 2, 2), names)
    cells, genes = names[:3], names[3:]
    return jax.shard_map(
        shards,
        mesh=finer,
        in_specs=(P(cells, genes), P(cells)),
        out_specs=(P(cells, genes), P(cells)),
        check_vma=False,
    )
```

```python
import functools

import jax
import jax.numpy as jnp
from jax import lax
from jax.experimental import pallas as pl
from jax.experimental.pallas import tpu as pltpu
from jax.sharding import Mesh
from jax.sharding import PartitionSpec as P

MESH = pl.DeviceIdType.MESH
BLOCK = 1024
SUB = 64
QUARTER = 256
LEVELS = 8190.0
CELLS_ALL = 65536.0


def kernel(
    counts_ref, library_ref, adj_ref, conn_ref,
    raw, xa, xb, rl, gr, gt, tt, f1, d1, r1, f2, d2, r2, zs, zr, xs, xr, ms, mr,
    st, sz, sx, sy, sc, sq, cm, cu, cw, rowv, cr, total_ref,
    load_sem, send_sem, recv_sem,
):
    x, zl, y = lax.axis_index("x"), lax.axis_index("zl"), lax.axis_index("y")
    zh, k = lax.axis_index("zh"), lax.axis_index("k")
    z = zh * 4 + zl
    spot = {"x": x, "y": y}
    mine = 2 * zh + k
    used = [0]
    started = []

    def remote(src, dst, where):
        n = used[0]
        used[0] += 1
        copy = pltpu.make_async_remote_copy(
            src_ref=src,
            dst_ref=dst,
            send_sem=send_sem.at[n],
            recv_sem=recv_sem.at[n],
            device_id=where,
            device_id_type=MESH,
        )
        copy.start()
        started.append(copy)
        return copy

    def along_z(hops):
        there = lax.rem(z + hops + 8, 8)
        return {"zh": there // 4, "zl": lax.rem(there, 4)}

    def hop(axis, by):
        return {axis: lax.rem(spot[axis] + by + 4, 4)}

    barrier = pltpu.get_barrier_semaphore()
    half_z = [{"zl": lax.rem(zl + d, 4)} for d in (3, 1, 2)]
    greeted = half_z + [{"k": 1 - k}, {"zh": 1 - zh}, {"zh": 1 - zh, "k": 1 - k}]
    greeted += [along_z(2), along_z(-2)]
    greeted += [hop(axis, d) for axis in ("x", "y") for d in (1, 2, 3)]
    for where in greeted:
        pl.semaphore_signal(barrier, inc=1, device_id=where, device_id_type=MESH)

    halves = (1 - zh, zh)
    loads = []
    for n in range(4):
        rows = pl.ds(pl.multiple_of(halves[n // 2] * 512 + (n % 2) * 256, 256), 256)
        loads.append(
            (rows, pltpu.make_async_copy(counts_ref.at[rows], raw.at[rows], load_sem.at[n]))
        )
        loads[-1][1].start()
    factor = 10000.0 / library_ref[...].astype(jnp.float32)
    cw[...] = jnp.broadcast_to(factor, (128, BLOCK)).T
    for n in range(4):
        rows, load = loads[n]
        load.wait()
        if n % 2 == 0:
            sq[...] = jnp.zeros_like(sq)

        def piece(i, carry, n=n):
            at = pl.ds(
                pl.multiple_of(halves[n // 2] * 512 + (n % 2) * 256 + i * 64, 64), 64
            )
            scale = cw[at]
            scale = jnp.concatenate([scale, scale], axis=1)
            for g in range(4):
                hi, lo = g % 2, g // 2
                lanes = pl.ds((2 * hi + lo) * QUARTER, QUARTER)
                value = jnp.log1p(raw[at, lanes].astype(jnp.float32) * scale)
                value = value.astype(jnp.bfloat16)
                xa[k, g, at] = value
                value = value.astype(jnp.float32).reshape(8, 8, QUARTER)
                sq[0, :, lanes] = sq[0, :, lanes] + jnp.sum(value, axis=0)
                sq[1, :, lanes] = sq[1, :, lanes] + jnp.sum(value * value, axis=0)
            return carry

        lax.fori_loop(0, 4, piece, 0)
        if n % 2:
            st[pl.ds(halves[n // 2], 1)] = jnp.sum(sq[0], axis=0, keepdims=True)
            st[pl.ds(2 + halves[n // 2], 1)] = jnp.sum(sq[1], axis=0, keepdims=True)
    pl.semaphore_wait(barrier, len(greeted))

    sz[zl] = st[...]
    stat_z = [remote(st, sz.at[zl], where) for where in half_z]
    partner_x = remote(xa.at[k], xa.at[k], {"k": 1 - k})
    far_half = pl.multiple_of((1 - zh) * 512, 512)

    ways = (along_z(2), along_z(-2))
    leg_one, leg_two = {}, {}

    def send_genes(i):
        leg_one[i] = [
            remote(
                xa.at[k, i, pl.ds(pl.multiple_of(far_half + 256 * f, 256), 256)],
                rl.at[f, i],
                ways[f],
            )
            for f in range(2)
        ]

    def forward(i):
        for c in leg_one[i]:
            c.wait_recv()
        leg_two[i] = [
            remote(rl.at[f, i], xb.at[k, i, pl.ds(256 * f, 256)], ways[f])
            for f in range(2)
        ]

    send_genes(0)
    send_genes(1)

    def to_partner(i):
        for c in leg_two[i]:
            c.wait_recv()
        return remote(xb.at[k, i], xb.at[k, i], {"k": 1 - k})

    ones = jnp.ones((BLOCK, 128), jnp.bfloat16)

    def raw_gram(a, lo):
        def body(hi, carry):
            t = 2 * a + hi
            turned = xa[a, 2 * lo + hi].T
            gt[lo, t] = jnp.dot(turned, ones, preferred_element_type=jnp.float32)
            for q in range(4):
                gr[lo, t, :, q * QUARTER : (q + 1) * QUARTER] = jnp.dot(
                    turned,
                    xa[k, (q % 2) * 2 + q // 2],
                    preferred_element_type=jnp.float32,
                )
            return carry

        lax.fori_loop(0, 2, body, 0)

    raw_gram(k, 0)
    raw_gram(k, 1)

    for c in stat_z:
        c.wait_recv()

    parts = [(sz[i, b : b + 1], sz[i, 2 + b : 3 + b]) for i in range(4) for b in range(2)]
    total = functools.reduce(jnp.add, [p[0] for p in parts])
    squares = functools.reduce(jnp.add, [p[1] for p in parts])
    mean = total * (1.0 / 4096.0)
    norms = [p[1] - 2.0 * mean * p[0] + 512.0 * mean * mean for p in parts]
    norm = functools.reduce(jnp.maximum, norms) * 1.0001 + squares * 2.5e-7 + 1e-2
    for i, v in enumerate((total, squares, jnp.sqrt(norm))):
        sx[x, i : i + 1] = v

    def spread(ref, axis):
        here = spot[axis]
        return [remote(ref.at[here], ref.at[here], hop(axis, d)) for d in (1, 3, 2)]

    def gathered(copies, ref, cells, out, slot):
        for c in copies:
            c.wait_recv()
        parts = [[ref[i, r : r + 1] for r in range(3)] for i in range(4)]
        total = parts[0][0] + parts[1][0] + parts[2][0] + parts[3][0]
        squares = parts[0][1] + parts[1][1] + parts[2][1] + parts[3][1]
        mean = total * (0.25 / cells)
        norms = [
            p[2] + (512.0**0.5) * jnp.abs(p[0] * (1.0 / cells) - mean) for p in parts
        ]
        norm = functools.reduce(jnp.maximum, norms)
        for i, v in enumerate((total, squares, norm)):
            out[slot, i : i + 1] = v

    copies = spread(sx, "x")
    partner_x.wait_recv()
    forward(0)
    raw_gram(1 - k, 0)
    gathered(copies, sx, 4096.0, sy, y)
    copies = spread(sy, "y")
    raw_gram(1 - k, 1)
    gathered(copies, sy, 16384.0, sc, mine)
    stat_core = remote(sc.at[mine], sc.at[mine], {"k": 1 - k})
    stat_far = [
        remote(sc.at[mine], sc.at[mine], {"zh": 1 - zh}),
        remote(sc.at[mine], sc.at[mine], {"zh": 1 - zh, "k": 1 - k}),
    ]
    forward(1)
    send_genes(2)
    send_genes(3)

    def columns(side):
        for a in range(2):
            b = 2 * side + a
            mean = sc[b, 0:1] * (1.0 / CELLS_ALL)
            unit = (LEVELS / 2.0) ** 0.5 / sc[b, 2:3]
            variance = sc[b, 1:2] * (1.0 / CELLS_ALL) - mean * mean
            rowv[b, 0:1] = mean
            rowv[b, 1:2] = unit
            rowv[b, 2:3] = lax.rsqrt(variance + 1e-05) / unit
            cm[b] = jnp.broadcast_to(mean, (128, BLOCK)).T
            cu[b] = jnp.broadcast_to(unit, (128, BLOCK)).T

    stat_core.wait_recv()
    columns(zh)
    own_mean, own_unit = rowv[mine, 0:1], rowv[mine, 1:2]
    for e, total in enumerate((st[0:1] + st[1:2], st[pl.ds(zh, 1)])):
        sq[e, 0:1] = own_mean * own_unit * (1.0 + e)
        sq[e, 1:2] = total * own_unit * (1.0 + e)
        sq[e, 2:3] = own_unit * (1.0 + e)

    wide = lambda v: jnp.concatenate([v, v], axis=1)

    def rounded(e, lo, q, a, hi, gram, factors):
        unit, off, mean = factors
        at = pl.ds(q * QUARTER, QUARTER)
        value = (
            gram * unit * sq[e, 2:3, at] - off * sq[e, 0:1, at] - mean * sq[e, 1:2, at]
        )
        value = jnp.clip(value, -LEVELS, LEVELS)
        code = jnp.round(value).astype(jnp.int32).astype(jnp.int16)
        rows = pl.ds(pl.multiple_of(hi * SUB, SUB), SUB)
        for c in range(2):
            part = code[:, c * 128 : (c + 1) * 128].reshape(4, SUB, 128)
            if q < 2:
                tt[2 * e + lo, q, 2 * a + c, :, rows] = part
            else:
                tt[2 * e + lo, q, :, pl.ds(2 * a + c, 1), rows] = part[:, None]

    def row_factors(e, lo, a, hi, total):
        side = lax.rem(zh + e, 2)
        first = pl.multiple_of((2 * hi + lo) * QUARTER, QUARTER)
        mean = cm[2 * side + a, pl.ds(first, QUARTER)]
        unit = cu[2 * side + a, pl.ds(first, QUARTER)]
        off = (total - (512.0 if e else 1024.0) * mean) * unit
        return wide(unit), wide(off), wide(mean * unit)

    def own_codes(lo, q):
        def body(t, carry):
            a, hi = t // 2, lax.rem(t, 2)
            factors = row_factors(0, lo, a, hi, gt[lo, t])
            gram = gr[lo, t, :, q * QUARTER : (q + 1) * QUARTER]
            rounded(0, lo, q, a, hi, gram, factors)
            return carry

        lax.fori_loop(0, 4, body, 0)

    def cross_codes(lo):
        def body(t, carry):
            a, hi = t // 2, lax.rem(t, 2)
            turned = xb[a, 2 * lo + hi].T
            total = jnp.dot(turned, ones[:512], preferred_element_type=jnp.float32)
            factors = row_factors(1, lo, a, hi, total)
            near = pl.ds(pl.multiple_of(zh * 512, 512), 512)
            for q in range(4):
                right = xa[k, (q % 2) * 2 + q // 2, near]
                gram = jnp.dot(turned, right, preferred_element_type=jnp.float32)
                rounded(1, lo, q, a, hi, gram, factors)
            return carry

        lax.fori_loop(0, 4, body, 0)

    axes = [("x", "y", -1), ("x", "y", 1), ("y", "x", -1), ("y", "x", 1)]

    def at4(axis, by):
        return lax.rem(spot[axis] + by + 4, 4)

    class Ring:
        def __init__(self, tile, axis, s, far, direct, relay):
            self.tile, self.axis, self.s = tile, axis, s
            self.far, self.direct, self.relay = far, direct, relay
            self.c_far = remote(tile(at4(axis, 2)), far, hop(axis, s))

        def send_direct(self):
            s = self.s
            self.c_direct = remote(
                self.tile(at4(self.axis, -s)), self.direct, hop(self.axis, -s)
            )

        def pass_on(self):
            self.c_far.wait_recv()
            here = self.tile(at4(self.axis, self.s))
            here[...] = here[...] + self.far[...]
            self.c_relay = remote(here, self.relay, hop(self.axis, self.s))

        def total(self):
            self.c_direct.wait_recv()
            self.c_relay.wait_recv()
            here = self.tile(spot[self.axis])
            return here[...] + self.direct[...] + self.relay[...]

    rings1, rings2 = {}, {}

    def p1(j, q):
        first, _, s = axes[q]
        rings1[j, q] = Ring(
            lambda d: tt.at[j, q, d], first, s, f1.at[j, q], d1.at[j, q], r1.at[j, q]
        )

    def p2(j):
        for q in range(4):
            rings1[j, q].pass_on()

    def p3(j):
        for q, (first, second, s) in enumerate(axes):
            total = rings1[j, q].total().astype(jnp.int32)
            here = spot[first]
            tt[j, q, here] = ((total + 2) >> 2).astype(jnp.int16)
            rings2[j, q] = Ring(
                lambda d, q=q, here=here: tt.at[j, q, here, d],
                second, s, f2.at[j, q], d2.at[j, q], r2.at[j, q],
            )
        for q in range(4):
            rings2[j, q].send_direct()

    def p4(j):
        for q in range(4):
            rings2[j, q].pass_on()

    last_sends = []

    def p5(j):
        e, lo = j // 2, j % 2
        for q in range(4):
            total = rings2[j, q].total()
            for hi in range(2):
                zs[j, hi, :, q * 128 : (q + 1) * 128] = total[hi * SUB : (hi + 1) * SUB]
        for hi in range(2):
            hand_over(zs.at[j, hi], zr.at[e, zl], {"zl": 2 * hi + lo}, 2 * hi + lo == zl, e * 4 + zl)

    def hand_over(src, dst, where, stays, slot):
        n = used[0]
        used[0] += 1
        copy = pltpu.make_async_remote_copy(
            src_ref=src,
            dst_ref=dst,
            send_sem=send_sem.at[n],
            recv_sem=recv_sem.at[LAST + slot],
            device_id=where,
            device_id_type=MESH,
        )

        @pl.when(jnp.logical_not(stays))
        def _():
            copy.start()

        @pl.when(stays)
        def _():
            dst[...] = src[...]

        last_sends.append((stays, copy))

    def arrival(src, dst, slot):
        return pltpu.make_async_remote_copy(
            src_ref=src,
            dst_ref=dst,
            send_sem=send_sem.at[0],
            recv_sem=recv_sem.at[LAST + slot],
            device_id={"k": 1 - k},
            device_id_type=MESH,
        )

    c_here = lax.rem(x, 2)

    def settle(e):
        for s in range(4):

            @pl.when(zl != s)
            def _(s=s):
                arrival(zs.at[0, 0], zr.at[e, s], e * 4 + s).wait_recv()

        for q in range(4):
            at = slice(q * 128, (q + 1) * 128)
            parts = [zr[e, s, :, at].astype(jnp.int32) for s in range(4)]
            code = (functools.reduce(jnp.add, parts) + 2) >> 2
            xs[e, :, at] = code.astype(jnp.int16)
            if e:
                low = lax.broadcasted_iota(jnp.int32, (32, 128), 1) < SUB
                part = code.astype(jnp.float32)
                top, bottom = part[:32], part[32:]
                even = jnp.where(low, top, pltpu.roll(bottom, SUB, 1))
                odd = jnp.where(low, pltpu.roll(top, SUB, 1), bottom)
                for half, v in enumerate((even, odd)):
                    ms[2 * q + half] = v.astype(jnp.int32).astype(jnp.int16)
        if e:
            for n in range(8):
                slot = used[0]
                used[0] += 1
                copy = pltpu.make_async_remote_copy(
                    src_ref=ms.at[n],
                    dst_ref=mr.at[zl * 4 + y],
                    send_sem=send_sem.at[slot],
                    recv_sem=recv_sem.at[LAST + 10 + zl * 4 + y],
                    device_id={
                        "x": mine, "zl": n // 2, "y": 2 * c_here + n % 2,
                        "zh": 1 - zh, "k": x // 2,
                    },
                    device_id_type=MESH,
                )
                copy.start()
                started.append(copy)
        to_x = 2 * lax.rem(zh + e, 2) + x // 2
        hand_over(xs.at[e], xr.at[c_here], {"x": to_x}, to_x == x, 8 + c_here)

    def directs(j):
        for q in range(4):
            rings1[j, q].send_direct()

    for lo in range(2):
        for q in range(4):
            own_codes(lo, q)
            p1(lo, q)
        directs(lo)
    p2(0)
    partner_b = [to_partner(0), to_partner(1)]
    for c in stat_far:
        c.wait_recv()
    columns(1 - zh)
    p2(1)
    forward(2)
    partner_b[0].wait_recv()
    partner_b[1].wait_recv()
    cross_codes(0)
    for q in range(4):
        p1(2, q)
    directs(2)
    p3(0)
    forward(3)
    cw[...] = jnp.broadcast_to(rowv[x, 2:3], (128, BLOCK)).T
    p3(1)
    p2(2)
    p4(0)
    p4(1)
    partner_b += [to_partner(2), to_partner(3)]
    partner_b[2].wait_recv()
    partner_b[3].wait_recv()
    cross_codes(1)
    for q in range(4):
        p1(3, q)
    directs(3)
    p3(2)
    p5(0)
    p5(1)
    p2(3)
    p4(2)
    p3(3)
    p5(2)
    p4(3)
    settle(0)
    p5(3)

    settle(1)

    for c in range(2):

        @pl.when(2 * lax.rem(x, 2) + c != x)
        def _(c=c):
            arrival(xs.at[0], xr.at[c], 8 + c).wait_recv()

        for q in range(4):
            first = q * QUARTER + c * 128
            part = xr[c, :, q * 128 : (q + 1) * 128].astype(jnp.int32)
            total_ref[:, first : first + 128] = 4.0 * part.astype(jnp.float32)

    @pl.when((x // 2) != zh)
    def _():
        for s in range(16):
            arrival(ms.at[0], mr.at[s], 10 + s).wait_recv()
        for m in range(8):
            pieces = []
            for s in (2 * m, 2 * m + 1):
                part = mr[s].astype(jnp.int32).astype(jnp.float32)
                pieces += [part, pltpu.roll(part, SUB, 1)]
            turned = jnp.concatenate(pieces, axis=0).T[:SUB]
            at = slice(m * 128, (m + 1) * 128)
            total_ref[:, at] = total_ref[:, at] * 0.5 + 2.0 * turned

    first = pl.multiple_of((zl * 4 + y) * SUB, SUB)
    weight = cw[pl.ds(first, SUB)] * (4.0 / CELLS_ALL)
    row = x * BLOCK + first + lax.broadcasted_iota(jnp.int32, (SUB, 128), 0)
    partial = jnp.zeros((SUB, 128), jnp.float32)
    for m in range(8):
        at = pl.ds(m * 128, 128)
        value = total_ref[:, at] * weight * rowv[mine, 2:3, at]
        square = value * value
        power = square * square * square
        lane = mine * BLOCK + m * 128 + lax.broadcasted_iota(jnp.int32, (SUB, 128), 1)
        power = jnp.where(row == lane, 0.0, power)
        adj_ref[:, at] = power
        partial = partial + power
    both = jnp.concatenate([partial, jnp.zeros_like(partial)], axis=0).T
    cr[3] = jnp.broadcast_to(jnp.sum(both, axis=0, keepdims=True), (8, 128))
    to = [{"k": 1 - k}, {"zh": 1 - zh}, {"k": 1 - k, "zh": 1 - zh}]
    ends = [remote(cr.at[3], cr.at[i], where) for i, where in enumerate(to)]
    for c in ends:
        c.wait_recv()
    conn_ref[...] = (cr[0] + cr[1] + cr[2] + cr[3])[0:1, :SUB]
    for c in started:
        c.wait_send()
    for stays, copy in last_sends:

        @pl.when(jnp.logical_not(stays))
        def _(copy=copy):
            copy.wait_send()

    assert used[0] <= LAST, used[0]


LAST = 190


def shards(counts, library):
    i16, f32, bf16 = jnp.int16, jnp.float32, jnp.bfloat16
    vmem = pl.BlockSpec(memory_space=pltpu.VMEM)
    wide_buffer = pltpu.VMEM((4, 4, 4, 128, 128), i16)
    small_buffer = pltpu.VMEM((4, 4, 128, 128), i16)
    adjacency, connectivity = pl.pallas_call(
        kernel,
        name="network",
        out_shape=(
            jax.ShapeDtypeStruct((SUB, BLOCK), f32),
            jax.ShapeDtypeStruct((1, SUB), f32),
        ),
        in_specs=[pl.BlockSpec(memory_space=pl.ANY), vmem],
        out_specs=(vmem, vmem),
        scratch_shapes=[
            pltpu.VMEM((BLOCK, BLOCK), jnp.int32),
            pltpu.VMEM((2, 4, BLOCK, QUARTER), bf16),
            pltpu.VMEM((2, 4, 512, QUARTER), bf16),
            pltpu.VMEM((2, 4, QUARTER, QUARTER), bf16),
            pltpu.VMEM((2, 4, QUARTER, BLOCK), f32),
            pltpu.VMEM((2, 4, QUARTER, 128), f32),
            pltpu.VMEM((4, 4, 4, 4, 128, 128), i16),
            wide_buffer, wide_buffer, wide_buffer,
            small_buffer, small_buffer, small_buffer,
            pltpu.VMEM((4, 2, SUB, 512), i16),
            pltpu.VMEM((2, 4, SUB, 512), i16),
            pltpu.VMEM((2, SUB, 512), i16),
            pltpu.VMEM((2, SUB, 512), i16),
            pltpu.VMEM((8, 32, 128), i16),
            pltpu.VMEM((16, 32, 128), i16),
            pltpu.VMEM((4, BLOCK), f32),
            pltpu.VMEM((4, 4, BLOCK), f32),
            pltpu.VMEM((4, 4, BLOCK), f32),
            pltpu.VMEM((4, 4, BLOCK), f32),
            pltpu.VMEM((4, 4, BLOCK), f32),
            pltpu.VMEM((2, 8, BLOCK), f32),
            pltpu.VMEM((4, BLOCK, 128), f32),
            pltpu.VMEM((4, BLOCK, 128), f32),
            pltpu.VMEM((BLOCK, 128), f32),
            pltpu.VMEM((4, 8, BLOCK), f32),
            pltpu.VMEM((4, 8, 128), f32),
            pltpu.VMEM((SUB, BLOCK), f32),
            pltpu.SemaphoreType.DMA((4,)),
            pltpu.SemaphoreType.DMA((LAST,)),
            pltpu.SemaphoreType.DMA((LAST + 26,)),
        ],
        compiler_params=pltpu.CompilerParams(
            collective_id=0, has_side_effects=True, vmem_limit_bytes=56 * 1024 * 1024
        ),
    )(counts, library.reshape(1, BLOCK))
    return adjacency, connectivity.reshape(SUB)


def solution(mesh):
    names = ("x", "zl", "y", "zh", "k")
    finer = Mesh(mesh.devices.reshape(4, 4, 4, 2, 2), names)
    cells, genes = names[:3], names[3:]
    return jax.shard_map(
        shards,
        mesh=finer,
        in_specs=(P(cells, genes), P(cells)),
        out_specs=(P(cells, genes), P(cells)),
        check_vma=False,
    )
```

```python
import functools

import jax
import jax.numpy as jnp
from jax import lax
from jax.experimental import pallas as pl
from jax.experimental.pallas import tpu as pltpu
from jax.sharding import Mesh
from jax.sharding import PartitionSpec as P

MESH = pl.DeviceIdType.MESH
BLOCK = 1024
SUB = 64
QUARTER = 256
LEVELS = 8190.0
CELLS_ALL = 65536.0


def kernel(
    counts_ref, library_ref, adj_ref, conn_ref,
    raw, xa, xb, rl, gr, gt, tt, f1, d1, r1, f2, d2, r2, zs, zr, xs, xr, ms, mr,
    st, sz, sx, sy, sc, sq, cm, cu, cw, rowv, cr, total_ref,
    load_sem, send_sem, recv_sem,
):
    x, zl, y = lax.axis_index("x"), lax.axis_index("zl"), lax.axis_index("y")
    zh, k = lax.axis_index("zh"), lax.axis_index("k")
    z = zh * 4 + zl
    spot = {"x": x, "y": y}
    mine = 2 * zh + k
    used = [0]
    started = []

    def remote(src, dst, where):
        n = used[0]
        used[0] += 1
        copy = pltpu.make_async_remote_copy(
            src_ref=src,
            dst_ref=dst,
            send_sem=send_sem.at[n],
            recv_sem=recv_sem.at[n],
            device_id=where,
            device_id_type=MESH,
        )
        copy.start()
        started.append(copy)
        return copy

    def along_z(hops):
        there = lax.rem(z + hops + 8, 8)
        return {"zh": there // 4, "zl": lax.rem(there, 4)}

    def hop(axis, by):
        return {axis: lax.rem(spot[axis] + by + 4, 4)}

    barrier = pltpu.get_barrier_semaphore()
    half_z = [{"zl": lax.rem(zl + d, 4)} for d in (3, 1, 2)]
    greeted = half_z + [{"k": 1 - k}, {"zh": 1 - zh}, {"zh": 1 - zh, "k": 1 - k}]
    greeted += [along_z(2), along_z(-2)]
    greeted += [hop(axis, d) for axis in ("x", "y") for d in (1, 2, 3)]
    for where in greeted:
        pl.semaphore_signal(barrier, inc=1, device_id=where, device_id_type=MESH)

    halves = (1 - zh, zh)
    loads = []
    for n in range(4):
        rows = pl.ds(pl.multiple_of(halves[n // 2] * 512 + (n % 2) * 256, 256), 256)
        loads.append(
            (rows, pltpu.make_async_copy(counts_ref.at[rows], raw.at[rows], load_sem.at[n]))
        )
        loads[-1][1].start()
    factor = 10000.0 / library_ref[...].astype(jnp.float32)
    cw[...] = jnp.broadcast_to(factor, (128, BLOCK)).T
    for n in range(4):
        rows, load = loads[n]
        load.wait()
        if n % 2 == 0:
            sq[...] = jnp.zeros_like(sq)

        def piece(i, carry, n=n):
            at = pl.ds(
                pl.multiple_of(halves[n // 2] * 512 + (n % 2) * 256 + i * 64, 64), 64
            )
            scale = cw[at]
            scale = jnp.concatenate([scale, scale], axis=1)
            for g in range(4):
                hi, lo = g % 2, g // 2
                lanes = pl.ds((2 * hi + lo) * QUARTER, QUARTER)
                value = jnp.log1p(raw[at, lanes].astype(jnp.float32) * scale)
                value = value.astype(jnp.bfloat16)
                xa[k, g, at] = value
                value = value.astype(jnp.float32).reshape(8, 8, QUARTER)
                sq[0, :, lanes] = sq[0, :, lanes] + jnp.sum(value, axis=0)
                sq[1, :, lanes] = sq[1, :, lanes] + jnp.sum(value * value, axis=0)
            return carry

        lax.fori_loop(0, 4, piece, 0)
        if n % 2:
            st[pl.ds(halves[n // 2], 1)] = jnp.sum(sq[0], axis=0, keepdims=True)
            st[pl.ds(2 + halves[n // 2], 1)] = jnp.sum(sq[1], axis=0, keepdims=True)
    pl.semaphore_wait(barrier, len(greeted))

    sz[zl] = st[...]
    stat_z = [remote(st, sz.at[zl], where) for where in half_z]
    partner_x = remote(xa.at[k], xa.at[k], {"k": 1 - k})
    far_half = pl.multiple_of((1 - zh) * 512, 512)

    ways = (along_z(2), along_z(-2))
    leg_one, leg_two = {}, {}

    def send_genes(i):
        leg_one[i] = [
            remote(
                xa.at[k, i, pl.ds(pl.multiple_of(far_half + 256 * f, 256), 256)],
                rl.at[f, i],
                ways[f],
            )
            for f in range(2)
        ]

    def forward(i):
        for c in leg_one[i]:
            c.wait_recv()
        leg_two[i] = [
            remote(rl.at[f, i], xb.at[k, i, pl.ds(256 * f, 256)], ways[f])
            for f in range(2)
        ]

    send_genes(0)
    send_genes(1)

    def to_partner(i):
        for c in leg_two[i]:
            c.wait_recv()
        return remote(xb.at[k, i], xb.at[k, i], {"k": 1 - k})

    ones = jnp.ones((BLOCK, 128), jnp.bfloat16)

    def raw_gram(a, lo):
        def body(hi, carry):
            t = 2 * a + hi
            turned = xa[a, 2 * lo + hi].T
            gt[lo, t] = jnp.dot(turned, ones, preferred_element_type=jnp.float32)
            for q in range(4):
                gr[lo, t, :, q * QUARTER : (q + 1) * QUARTER] = jnp.dot(
                    turned,
                    xa[k, (q % 2) * 2 + q // 2],
                    preferred_element_type=jnp.float32,
                )
            return carry

        lax.fori_loop(0, 2, body, 0)

    raw_gram(k, 0)
    raw_gram(k, 1)

    for c in stat_z:
        c.wait_recv()

    parts = [(sz[i, b : b + 1], sz[i, 2 + b : 3 + b]) for i in range(4) for b in range(2)]
    total = functools.reduce(jnp.add, [p[0] for p in parts])
    squares = functools.reduce(jnp.add, [p[1] for p in parts])
    mean = total * (1.0 / 4096.0)
    norms = [p[1] - 2.0 * mean * p[0] + 512.0 * mean * mean for p in parts]
    norm = functools.reduce(jnp.maximum, norms) * 1.0001 + squares * 2.5e-7 + 1e-2
    for i, v in enumerate((total, squares, jnp.sqrt(norm))):
        sx[x, i : i + 1] = v

    def spread(ref, axis):
        here = spot[axis]
        return [remote(ref.at[here], ref.at[here], hop(axis, d)) for d in (1, 3, 2)]

    def gathered(copies, ref, cells, out, slot):
        for c in copies:
            c.wait_recv()
        parts = [[ref[i, r : r + 1] for r in range(3)] for i in range(4)]
        total = parts[0][0] + parts[1][0] + parts[2][0] + parts[3][0]
        squares = parts[0][1] + parts[1][1] + parts[2][1] + parts[3][1]
        mean = total * (0.25 / cells)
        norms = [
            p[2] + (512.0**0.5) * jnp.abs(p[0] * (1.0 / cells) - mean) for p in parts
        ]
        norm = functools.reduce(jnp.maximum, norms)
        for i, v in enumerate((total, squares, norm)):
            out[slot, i : i + 1] = v

    copies = spread(sx, "x")
    partner_x.wait_recv()
    forward(0)
    raw_gram(1 - k, 0)
    gathered(copies, sx, 4096.0, sy, y)
    copies = spread(sy, "y")
    raw_gram(1 - k, 1)
    gathered(copies, sy, 16384.0, sc, mine)
    stat_core = remote(sc.at[mine], sc.at[mine], {"k": 1 - k})
    stat_far = [
        remote(sc.at[mine], sc.at[mine], {"zh": 1 - zh}),
        remote(sc.at[mine], sc.at[mine], {"zh": 1 - zh, "k": 1 - k}),
    ]
    forward(1)
    send_genes(2)
    send_genes(3)

    def columns(side):
        for a in range(2):
            b = 2 * side + a
            mean = sc[b, 0:1] * (1.0 / CELLS_ALL)
            unit = (LEVELS / 2.0) ** 0.5 / sc[b, 2:3]
            variance = sc[b, 1:2] * (1.0 / CELLS_ALL) - mean * mean
            rowv[b, 0:1] = mean
            rowv[b, 1:2] = unit
            rowv[b, 2:3] = lax.rsqrt(variance + 1e-05) / unit
            cm[b] = jnp.broadcast_to(mean, (128, BLOCK)).T
            cu[b] = jnp.broadcast_to(unit, (128, BLOCK)).T

    stat_core.wait_recv()
    columns(zh)
    own_mean, own_unit = rowv[mine, 0:1], rowv[mine, 1:2]
    for e, total in enumerate((st[0:1] + st[1:2], st[pl.ds(zh, 1)])):
        sq[e, 0:1] = own_mean * own_unit * (1.0 + e)
        sq[e, 1:2] = total * own_unit * (1.0 + e)
        sq[e, 2:3] = own_unit * (1.0 + e)

    wide = lambda v: jnp.concatenate([v, v], axis=1)

    def rounded(e, lo, q, a, hi, gram, factors):
        unit, off, mean = factors
        at = pl.ds(q * QUARTER, QUARTER)
        value = (
            gram * unit * sq[e, 2:3, at] - off * sq[e, 0:1, at] - mean * sq[e, 1:2, at]
        )
        value = jnp.clip(value, -LEVELS, LEVELS)
        code = jnp.round(value).astype(jnp.int32).astype(jnp.int16)
        rows = pl.ds(pl.multiple_of(hi * SUB, SUB), SUB)
        for c in range(2):
            part = code[:, c * 128 : (c + 1) * 128].reshape(4, SUB, 128)
            if q < 2:
                tt[2 * e + lo, q, 2 * a + c, :, rows] = part
            else:
                tt[2 * e + lo, q, :, pl.ds(2 * a + c, 1), rows] = part[:, None]

    def row_factors(e, lo, a, hi, total):
        side = lax.rem(zh + e, 2)
        first = pl.multiple_of((2 * hi + lo) * QUARTER, QUARTER)
        mean = cm[2 * side + a, pl.ds(first, QUARTER)]
        unit = cu[2 * side + a, pl.ds(first, QUARTER)]
        off = (total - (512.0 if e else 1024.0) * mean) * unit
        return wide(unit), wide(off), wide(mean * unit)

    def own_codes(lo, q):
        def body(t, carry):
            a, hi = t // 2, lax.rem(t, 2)
            factors = row_factors(0, lo, a, hi, gt[lo, t])
            gram = gr[lo, t, :, q * QUARTER : (q + 1) * QUARTER]
            rounded(0, lo, q, a, hi, gram, factors)
            return carry

        lax.fori_loop(0, 4, body, 0)

    def cross_codes(lo):
        def body(t, carry):
            a, hi = t // 2, lax.rem(t, 2)
            turned = xb[a, 2 * lo + hi].T
            total = jnp.dot(turned, ones[:512], preferred_element_type=jnp.float32)
            factors = row_factors(1, lo, a, hi, total)
            near = pl.ds(pl.multiple_of(zh * 512, 512), 512)
            for q in range(4):
                right = xa[k, (q % 2) * 2 + q // 2, near]
                gram = jnp.dot(turned, right, preferred_element_type=jnp.float32)
                rounded(1, lo, q, a, hi, gram, factors)
            return carry

        lax.fori_loop(0, 4, body, 0)

    axes = [("x", "y", -1), ("x", "y", 1), ("y", "x", -1), ("y", "x", 1)]

    def at4(axis, by):
        return lax.rem(spot[axis] + by + 4, 4)

    class Ring:
        def __init__(self, tile, axis, s, far, direct, relay):
            self.tile, self.axis, self.s = tile, axis, s
            self.far, self.direct, self.relay = far, direct, relay
            self.c_far = remote(tile(at4(axis, 2)), far, hop(axis, s))

        def send_direct(self):
            s = self.s
            self.c_direct = remote(
                self.tile(at4(self.axis, -s)), self.direct, hop(self.axis, -s)
            )

        def pass_on(self):
            self.c_far.wait_recv()
            here = self.tile(at4(self.axis, self.s))
            here[...] = here[...] + self.far[...]
            self.c_relay = remote(here, self.relay, hop(self.axis, self.s))

        def total(self):
            self.c_direct.wait_recv()
            self.c_relay.wait_recv()
            here = self.tile(spot[self.axis])
            return here[...] + self.direct[...] + self.relay[...]

    rings1, rings2 = {}, {}

    def p1(j, q):
        first, _, s = axes[q]
        rings1[j, q] = Ring(
            lambda d: tt.at[j, q, d], first, s, f1.at[j, q], d1.at[j, q], r1.at[j, q]
        )

    def p2(j):
        for q in range(4):
            rings1[j, q].pass_on()

    def p3(j):
        for q, (first, second, s) in enumerate(axes):
            total = rings1[j, q].total().astype(jnp.int32)
            here = spot[first]
            tt[j, q, here] = ((total + 2) >> 2).astype(jnp.int16)
            rings2[j, q] = Ring(
                lambda d, q=q, here=here: tt.at[j, q, here, d],
                second, s, f2.at[j, q], d2.at[j, q], r2.at[j, q],
            )
        for q in range(4):
            rings2[j, q].send_direct()

    def p4(j):
        for q in range(4):
            rings2[j, q].pass_on()

    last_sends = []

    def p5(j):
        e, lo = j // 2, j % 2
        for q in range(4):
            total = rings2[j, q].total()
            for hi in range(2):
                zs[j, hi, :, q * 128 : (q + 1) * 128] = total[hi * SUB : (hi + 1) * SUB]
        for hi in range(2):
            hand_over(zs.at[j, hi], zr.at[e, zl], {"zl": 2 * hi + lo}, 2 * hi + lo == zl, e * 4 + zl)

    def hand_over(src, dst, where, stays, slot):
        n = used[0]
        used[0] += 1
        copy = pltpu.make_async_remote_copy(
            src_ref=src,
            dst_ref=dst,
            send_sem=send_sem.at[n],
            recv_sem=recv_sem.at[LAST + slot],
            device_id=where,
            device_id_type=MESH,
        )

        @pl.when(jnp.logical_not(stays))
        def _():
            copy.start()

        @pl.when(stays)
        def _():
            dst[...] = src[...]

        last_sends.append((stays, copy))

    def arrival(src, dst, slot):
        return pltpu.make_async_remote_copy(
            src_ref=src,
            dst_ref=dst,
            send_sem=send_sem.at[0],
            recv_sem=recv_sem.at[LAST + slot],
            device_id={"k": 1 - k},
            device_id_type=MESH,
        )

    c_here = lax.rem(x, 2)

    def settle(e):
        for s in range(4):

            @pl.when(zl != s)
            def _(s=s):
                arrival(zs.at[0, 0], zr.at[e, s], e * 4 + s).wait_recv()

        for q in range(4):
            at = slice(q * 128, (q + 1) * 128)
            parts = [zr[e, s, :, at].astype(jnp.int32) for s in range(4)]
            code = (functools.reduce(jnp.add, parts) + 2) >> 2
            xs[e, :, at] = code.astype(jnp.int16)
            if e:
                low = lax.broadcasted_iota(jnp.int32, (32, 128), 1) < SUB
                part = code.astype(jnp.float32)
                top, bottom = part[:32], part[32:]
                even = jnp.where(low, top, pltpu.roll(bottom, SUB, 1))
                odd = jnp.where(low, pltpu.roll(top, SUB, 1), bottom)
                for half, v in enumerate((even, odd)):
                    ms[2 * q + half] = v.astype(jnp.int32).astype(jnp.int16)
        if e:
            for n in range(8):
                slot = used[0]
                used[0] += 1
                copy = pltpu.make_async_remote_copy(
                    src_ref=ms.at[n],
                    dst_ref=mr.at[zl * 4 + y],
                    send_sem=send_sem.at[slot],
                    recv_sem=recv_sem.at[LAST + 10 + zl * 4 + y],
                    device_id={
                        "x": mine, "zl": n // 2, "y": 2 * c_here + n % 2,
                        "zh": 1 - zh, "k": x // 2,
                    },
                    device_id_type=MESH,
                )
                copy.start()
                started.append(copy)
        to_x = 2 * lax.rem(zh + e, 2) + x // 2
        hand_over(xs.at[e], xr.at[c_here], {"x": to_x}, to_x == x, 8 + c_here)

    def directs(j):
        for q in range(4):
            rings1[j, q].send_direct()

    for lo in range(2):
        for q in range(4):
            own_codes(lo, q)
            p1(lo, q)
        directs(lo)
    p2(0)
    partner_b = [to_partner(0), to_partner(1)]
    for c in stat_far:
        c.wait_recv()
    columns(1 - zh)
    p2(1)
    forward(2)
    partner_b[0].wait_recv()
    partner_b[1].wait_recv()
    cross_codes(0)
    for q in range(4):
        p1(2, q)
    directs(2)
    p3(0)
    forward(3)
    cw[...] = jnp.broadcast_to(rowv[x, 2:3], (128, BLOCK)).T
    p3(1)
    p2(2)
    p4(0)
    p4(1)
    partner_b += [to_partner(2), to_partner(3)]
    partner_b[2].wait_recv()
    partner_b[3].wait_recv()
    cross_codes(1)
    for q in range(4):
        p1(3, q)
    directs(3)
    p3(2)
    p5(0)
    p5(1)
    p2(3)
    p4(2)
    p3(3)
    p5(2)
    p4(3)
    settle(0)
    p5(3)

    settle(1)

    for c in range(2):

        @pl.when(2 * lax.rem(x, 2) + c != x)
        def _(c=c):
            arrival(xs.at[0], xr.at[c], 8 + c).wait_recv()

        for q in range(4):
            first = q * QUARTER + c * 128
            part = xr[c, :, q * 128 : (q + 1) * 128].astype(jnp.int32)
            total_ref[:, first : first + 128] = 4.0 * part.astype(jnp.float32)

    @pl.when((x // 2) != zh)
    def _():
        for s in range(16):
            arrival(ms.at[0], mr.at[s], 10 + s).wait_recv()
        for m in range(8):
            pieces = []
            for s in (2 * m, 2 * m + 1):
                part = mr[s].astype(jnp.int32).astype(jnp.float32)
                pieces += [part, pltpu.roll(part, SUB, 1)]
            turned = jnp.concatenate(pieces, axis=0).T[:SUB]
            at = slice(m * 128, (m + 1) * 128)
            total_ref[:, at] = total_ref[:, at] * 0.5 + 2.0 * turned

    first = pl.multiple_of((zl * 4 + y) * SUB, SUB)
    weight = cw[pl.ds(first, SUB)] * (4.0 / CELLS_ALL)
    row = x * BLOCK + first + lax.broadcasted_iota(jnp.int32, (SUB, 128), 0)
    partial = jnp.zeros((SUB, 128), jnp.float32)
    for m in range(8):
        at = pl.ds(m * 128, 128)
        value = total_ref[:, at] * weight * rowv[mine, 2:3, at]
        square = value * value
        power = square * square * square
        lane = mine * BLOCK + m * 128 + lax.broadcasted_iota(jnp.int32, (SUB, 128), 1)
        power = jnp.where(row == lane, 0.0, power)
        adj_ref[:, at] = power
        partial = partial + power
    both = jnp.concatenate([partial, jnp.zeros_like(partial)], axis=0).T
    cr[3] = jnp.broadcast_to(jnp.sum(both, axis=0, keepdims=True), (8, 128))
    to = [{"k": 1 - k}, {"zh": 1 - zh}, {"k": 1 - k, "zh": 1 - zh}]
    ends = [remote(cr.at[3], cr.at[i], where) for i, where in enumerate(to)]
    for c in ends:
        c.wait_recv()
    conn_ref[...] = (cr[0] + cr[1] + cr[2] + cr[3])[0:1, :SUB]
    for c in started:
        c.wait_send()
    for stays, copy in last_sends:

        @pl.when(jnp.logical_not(stays))
        def _(copy=copy):
            copy.wait_send()

    assert used[0] <= LAST, used[0]


LAST = 190


def shards(counts, library):
    i16, f32, bf16 = jnp.int16, jnp.float32, jnp.bfloat16
    vmem = pl.BlockSpec(memory_space=pltpu.VMEM)
    wide_buffer = pltpu.VMEM((4, 4, 4, 128, 128), i16)
    small_buffer = pltpu.VMEM((4, 4, 128, 128), i16)
    adjacency, connectivity = pl.pallas_call(
        kernel,
        name="network",
        out_shape=(
            jax.ShapeDtypeStruct((SUB, BLOCK), f32),
            jax.ShapeDtypeStruct((1, SUB), f32),
        ),
        in_specs=[pl.BlockSpec(memory_space=pltpu.HBM), vmem],
        out_specs=(vmem, vmem),
        scratch_shapes=[
            pltpu.VMEM((BLOCK, BLOCK), jnp.int32),
            pltpu.VMEM((2, 4, BLOCK, QUARTER), bf16),
            pltpu.VMEM((2, 4, 512, QUARTER), bf16),
            pltpu.VMEM((2, 4, QUARTER, QUARTER), bf16),
            pltpu.VMEM((2, 4, QUARTER, BLOCK), f32),
            pltpu.VMEM((2, 4, QUARTER, 128), f32),
            pltpu.VMEM((4, 4, 4, 4, 128, 128), i16),
            wide_buffer, wide_buffer, wide_buffer,
            small_buffer, small_buffer, small_buffer,
            pltpu.VMEM((4, 2, SUB, 512), i16),
            pltpu.VMEM((2, 4, SUB, 512), i16),
            pltpu.VMEM((2, SUB, 512), i16),
            pltpu.VMEM((2, SUB, 512), i16),
            pltpu.VMEM((8, 32, 128), i16),
            pltpu.VMEM((16, 32, 128), i16),
            pltpu.VMEM((4, BLOCK), f32),
            pltpu.VMEM((4, 4, BLOCK), f32),
            pltpu.VMEM((4, 4, BLOCK), f32),
            pltpu.VMEM((4, 4, BLOCK), f32),
            pltpu.VMEM((4, 4, BLOCK), f32),
            pltpu.VMEM((2, 8, BLOCK), f32),
            pltpu.VMEM((4, BLOCK, 128), f32),
            pltpu.VMEM((4, BLOCK, 128), f32),
            pltpu.VMEM((BLOCK, 128), f32),
            pltpu.VMEM((4, 8, BLOCK), f32),
            pltpu.VMEM((4, 8, 128), f32),
            pltpu.VMEM((SUB, BLOCK), f32),
            pltpu.SemaphoreType.DMA((4,)),
            pltpu.SemaphoreType.DMA((LAST,)),
            pltpu.SemaphoreType.DMA((LAST + 26,)),
        ],
        compiler_params=pltpu.CompilerParams(
            collective_id=0, has_side_effects=True, vmem_limit_bytes=48 * 1024 * 1024
        ),
    )(counts, library.reshape(1, BLOCK))
    return adjacency, connectivity.reshape(SUB)


def solution(mesh):
    names = ("x", "zl", "y", "zh", "k")
    finer = Mesh(mesh.devices.reshape(4, 4, 4, 2, 2), names)
    cells, genes = names[:3], names[3:]
    return jax.shard_map(
        shards,
        mesh=finer,
        in_specs=(P(cells, genes), P(cells)),
        out_specs=(P(cells, genes), P(cells)),
        check_vma=False,
    )
```
